768 devices in a mesh: rep: 192 (over y, x, z_lo), sp: 4 (over z_hi, core).
Axes of the slice: x: 4, y: 8, z: 12 (z_hi: 2, z_lo: 6; z = z_hi * 6 + z_lo), core: 2. Of those that a mesh axis runs over, the one named last changes fastest.
Arguments:
- field: bfloat16 [192, 128, 100, 128], P('rep', 'sp'), may hold values from -6 to 6
- send_blocks: int32 [4, 4, 8], P('sp'), may hold values from 0 to 31
- send_count: int32 [4, 4], P('sp'), may hold values from 1 to 8, as said below
- regrid_weights: bfloat16 [32, 8, 128, 128], P('sp'), may hold values from -0.1875 to 0.1875
- tile_slot: int32 [32, 8], P('sp'), may hold values from 0 to 31
- edge_inputs: bfloat16 [294912, 1536], P(('rep', 'sp')), may hold values from -24 to 24
- cotangent: bfloat16 [294912, 512], P(('rep', 'sp')), may hold values from -0.15625 to 0.15625
Outputs:
- hidden: bfloat16 [192, 32, 100, 128], P('rep', 'sp')
- weight_grad: float32 [1536, 512], P(('rep', 'sp'))
The draws below stay inside these ranges and needn't reach their ends.
Inputs may be any that keep to these rules, and one draw needn't show every extreme that they name: `send_count`: every count is at most 8, and some pair of shards has exactly 8 in every draw.
All inputs are finite; a program needn't handle non-finite values.
Results may differ from the reference program's by a relative error of at most 0.001.
Values may be sent and summed in bfloat16 or wider, within the bound.
A program may use at most 32 MiB of HBM per device.

```python
import jax
import jax.numpy as jnp
from jax import lax

CHANNELS = 100
HID = 512
BLK = 128
NODE_TILE = 128
READS = 8
BLOCKS_DEV = 32
PER = 8
EDGE_DEV = 384
SHARDS = 4
REPLICAS = 192
BLOCKS = 128
TILES = 32
SLOTS = 32
IN = 1536
EDGES = 294912
N_REP = 192
N_SP = 4


def draw_send_count(key, part):
    base_key = jax.random.fold_in(key, 11)
    first_key, second_key = jax.random.split(base_key)
    counts = jax.random.randint(first_key, (SHARDS * SHARDS,), 1, PER + 1)
    chosen = jax.random.randint(second_key, (), 0, SHARDS * SHARDS)
    counts = jnp.where(jnp.arange(SHARDS * SHARDS) == chosen, PER, counts)
    return counts.reshape(SHARDS, SHARDS).astype(jnp.int32)


def with_ends(array, stream_key, smallest, largest):
    shape = array.shape
    place = [jax.random.randint(jax.random.fold_in(stream_key, axis), (), 0, shape[axis]) for axis in range(len(shape))]
    array = array.at[tuple(place)].set(smallest)
    longest = shape.index(max(shape))
    place[longest] = (place[longest] + 1) % shape[longest]
    return array.at[tuple(place)].set(largest)


def raised(entries, key, source, target, blocks, factor):
    def block_of(position):
        return (jnp.arange(entries.shape[position]) // (entries.shape[position] // blocks)).reshape((-1,) + (1,) * (entries.ndim - 1 - position))

    one_side = jax.random.permutation(key, blocks)[block_of(target)]
    second = (block_of(target) + blocks // 2) % blocks
    return jnp.where((block_of(source) == one_side) | (block_of(source) == second), factor * entries, entries)


def levels(key, dims, cuts, smallest, high):
    factor_of, own = 1.0, jax.random.fold_in(key, 6)
    for axis_at, shards_of in cuts:
        draws = jnp.exp(jax.random.uniform(jax.random.fold_in(own, axis_at), (shards_of,), jnp.float32, smallest / len(cuts), high / len(cuts)))
        factor_of = factor_of * jnp.repeat(draws, dims[axis_at] // shards_of).reshape([-1 if axis == axis_at else 1 for axis in range(len(dims))])
    return factor_of


def gaussian(key, dims, width, reach, cuts=(), kind=jnp.bfloat16):
    values = jax.random.normal(key, dims, jnp.float32) * width
    if len(cuts) > 0:
        values = levels(key, dims, cuts, -0.22, 0.18) * values
    return jnp.clip(values, min=-reach, max=reach).astype(kind)


def gaussian_with(rng, dims, scale, bound, cuts, heavy, kind=jnp.bfloat16):
    drawn = scale * jax.random.normal(rng, dims, jnp.float32)
    if cuts:
        drawn = drawn * levels(rng, dims, cuts, -0.22, 0.18)
    return jnp.clip(raised(drawn, jax.random.fold_in(rng, 3), *heavy), -bound, bound).astype(kind)


def setup_inputs(seed: int = 0) -> dict:
    key_of = jax.random.split(jax.random.key(seed), 8)
    return {
        "field": gaussian(key_of[0], (REPLICAS, BLOCKS, CHANNELS, BLK), 1.0, 6.0, ((0, 192), (1, 4))),
        "send_blocks": with_ends(jax.random.randint(key_of[1], (SHARDS, SHARDS, PER), 0, BLOCKS_DEV), jax.random.fold_in(key_of[1], 1), 0, BLOCKS_DEV - 1).astype(jnp.int32),
        "send_count": draw_send_count(jax.random.fold_in(key_of[7], 71), 0),
        "regrid_weights": gaussian(key_of[3], (TILES, READS, BLK, NODE_TILE), (READS * BLK) ** -0.5, 0.1875, ((0, 4),)),
        "tile_slot": with_ends(jax.random.randint(key_of[4], (TILES, READS), 0, SLOTS), jax.random.fold_in(key_of[4], 1), 0, SLOTS - 1).astype(jnp.int32),
        "edge_inputs": gaussian_with(key_of[5], (EDGES, IN), 1.0, 24.0, ((0, 768),), (0, 1, 768, 6.0)),
        "cotangent": gaussian(key_of[6], (EDGES, HID), (EDGE_DEV * N_SP) ** -0.5, 0.15625, ((0, 768),)),
    }


def reference(field, send_blocks, send_count, regrid_weights, tile_slot, edge_inputs, cotangent):
    shards = send_blocks.shape[0]
    slots_each = send_blocks.shape[2]
    blocks_dev = field.shape[1] // shards
    tiles_dev = tile_slot.shape[0] // shards
    reads = tile_slot.shape[1]
    source = jnp.arange(shards, dtype=jnp.int32)
    global_block = source[:, None, None] * blocks_dev + send_blocks
    alive_mask = jnp.arange(slots_each, dtype=jnp.int32)[None, None, :] < send_count[:, :, None]
    global_block = jnp.transpose(global_block, (1, 0, 2)).reshape(shards, shards * slots_each)
    alive_mask = jnp.transpose(alive_mask, (1, 0, 2)).reshape(shards, shards * slots_each)
    slot_index = tile_slot.reshape(shards, tiles_dev, reads)
    weight_tiles = regrid_weights.reshape(shards, tiles_dev, reads, BLK, NODE_TILE)

    def one_sample(sample):
        def one_shard(pieces):
            blocks_read, alive, slots, weights = pieces
            received = jnp.where(alive[:, None, None], sample[blocks_read], jnp.zeros((), jnp.bfloat16))
            picked = received[slots]
            result = jnp.einsum("tbcx,tbxn->tcn", picked.astype(jnp.float32), weights.astype(jnp.float32))
            return result.astype(jnp.bfloat16)

        outcome = lax.map(one_shard, (global_block, alive_mask, slot_index, weight_tiles))
        return outcome.reshape(shards * tiles_dev, CHANNELS, NODE_TILE)

    hidden = lax.map(one_sample, field)

    groups = N_REP * N_SP
    edge_groups = edge_inputs.reshape(groups, edge_inputs.shape[0] // groups, edge_inputs.shape[1])
    cot_groups = cotangent.reshape(groups, cotangent.shape[0] // groups, cotangent.shape[1])

    def accumulate(carry, pieces):
        left, right = pieces
        product = lax.dot_general(left, right, (((0,), (0,)), ((), ())), preferred_element_type=jnp.float32)
        return carry + product, None

    start_grad = jnp.zeros((edge_inputs.shape[1], cotangent.shape[1]), jnp.float32)
    weight_grad, unused = lax.scan(accumulate, start_grad, (edge_groups, cot_groups))
    return hidden, weight_grad
```

```python
import jax
import jax.numpy as jnp
from jax import lax
from jax.experimental import pallas as pl
from jax.experimental.pallas import tpu as pltpu
from jax.sharding import Mesh
from jax.sharding import PartitionSpec as P

AXES = ("y", "x", "zl", "zh", "c")
NY, NX, NZL, NZH, NC = 8, 4, 6, 2, 2
NZ = NZL * NZH
ROWS = 48
XROWS = 40
MESH = pl.DeviceIdType.MESH


def kernel(
    blocks_ref, count_ref, slot_ref, field_hbm, weights_hbm, edges_hbm, cot_hbm,
    hidden_ref, grad_ref,
    field, weights, edges, cot, outgoing, pool,
    part, given, chip, from_x, sum_x, from_y, last_y, sum_y, last_x, total, to_z, from_z,
    in_sem, a_send, a_recv, d_send, d_recv, x_send, x_recv, y_send, y_recv,
    u_send, u_recv, v_send, v_recv, z_send, z_recv,
):
    y, x = lax.axis_index("y"), lax.axis_index("x")
    zl, zh, c = lax.axis_index("zl"), lax.axis_index("zh"), lax.axis_index("c")
    z = zh * NZL + zl
    own = zh * NC + c
    half = cot.shape[1] // 2

    def at(dy=0, dx=0, dz=0, dc=0):
        other = lax.rem(z + dz, NZ)
        return (
            lax.rem(y + dy, NY), lax.rem(x + dx, NX),
            lax.rem(other, NZL), lax.div(other, NZL), lax.rem(c + dc, NC),
        )

    loads = [
        pltpu.make_async_copy(field_hbm.at[0], field, in_sem.at[0]),
        pltpu.make_async_copy(edges_hbm, edges, in_sem.at[1]),
        pltpu.make_async_copy(cot_hbm, cot, in_sem.at[2]),
        pltpu.make_async_copy(weights_hbm, weights, in_sem.at[3]),
    ]
    for load in loads:
        load.start()

    barrier = pltpu.get_barrier_semaphore()

    def greet(**offset):
        pl.semaphore_signal(barrier, inc=1, device_id=at(**offset), device_id_type=MESH)

    def greet_z(k, carry):
        greet(dz=k)
        greet(dz=k, dc=1)
        return carry

    def greet_y(k, carry):
        greet(dy=k)
        return carry

    lax.fori_loop(1, NZ, greet_z, 0)
    lax.fori_loop(1, NY, greet_y, 0)
    for k in range(1, NX):
        greet(dx=k)
    greet(dc=1)

    loads[0].wait()

    def picked(shard, j):
        block = field[blocks_ref[0, shard, j]]
        return jnp.where(j < count_ref[0, shard], block, jnp.zeros_like(block))

    shard_of = [lax.rem(zh + k // 2, NZH) * NC + lax.rem(c + k % 2, NC) for k in range(4)]

    def gather(j, carry):
        for k in (2, 3, 1):
            outgoing[k - 1, j] = picked(shard_of[k], j)
        pool[own * 8 + j] = picked(own, j)
        return carry

    lax.fori_loop(0, 8, gather, 0)

    loads[1].wait()
    loads[2].wait()
    for k in range(4):
        piece = lax.dot_general(
            edges[:, k * 384 : (k + 1) * 384], cot[...], (((0,), (0,)), ((), ())),
            preferred_element_type=jnp.float32,
        )
        for h in range(2):
            part[h, 2 * k : 2 * k + 2] = piece[:, h * half : (h + 1) * half].reshape(2, NX, ROWS, half)

    pl.semaphore_wait(barrier, 2 * (NZ - 1) + (NY - 1) + (NX - 1) + 1)

    def block_copy(k):
        return pltpu.make_async_remote_copy(
            src_ref=outgoing.at[k - 1], dst_ref=pool.at[pl.ds(own * 8, 8)],
            send_sem=a_send.at[k - 1], recv_sem=a_recv.at[k - 1],
            device_id=at(dz=NZL * (k // 2), dc=k % 2), device_id_type=MESH,
        )

    for k in (2, 3, 1):
        block_copy(k).start()

    def away(k):
        return 4 + lax.div(k, 2) * (1 - 2 * lax.rem(k, 2)) - lax.rem(k, 2)

    def core_copy(dy):
        return pltpu.make_async_remote_copy(
            src_ref=part.at[1 - c, lax.rem(y + dy, NY)], dst_ref=given.at[dy],
            send_sem=d_send.at[dy], recv_sem=d_recv.at[dy], device_id=at(dc=1), device_id_type=MESH,
        )

    def x_copy(dx, dy):
        return pltpu.make_async_remote_copy(
            src_ref=chip.at[dy, lax.rem(x + dx, NX), pl.ds(0, XROWS)], dst_ref=from_x.at[dx - 1, dy],
            send_sem=x_send.at[dx - 1, dy], recv_sem=x_recv.at[dx - 1, dy],
            device_id=at(dx=dx), device_id_type=MESH,
        )

    def y_copy(dy):
        return pltpu.make_async_remote_copy(
            src_ref=sum_x.at[dy], dst_ref=from_y.at[dy], send_sem=y_send.at[dy], recv_sem=y_recv.at[dy],
            device_id=at(dy=dy), device_id_type=MESH,
        )

    def u_copy(dy):
        return pltpu.make_async_remote_copy(
            src_ref=chip.at[dy, :, pl.ds(XROWS, ROWS - XROWS)], dst_ref=last_y.at[dy],
            send_sem=u_send.at[dy], recv_sem=u_recv.at[dy], device_id=at(dy=dy), device_id_type=MESH,
        )

    def v_copy(dx):
        return pltpu.make_async_remote_copy(
            src_ref=sum_y.at[lax.rem(x + dx, NX)], dst_ref=last_x.at[dx - 1],
            send_sem=v_send.at[dx - 1], recv_sem=v_recv.at[dx - 1], device_id=at(dx=dx), device_id_type=MESH,
        )

    def start_core(k, carry):
        core_copy(away(k)).start()
        return carry

    lax.fori_loop(0, NY, start_core, 0)

    def send_x(k):
        dy = away(k)
        for dx in (2, 1, 3):
            x_copy(dx, dy).start()

        @pl.when(dy > 0)
        def _():
            u_copy(dy).start()

    def over_cores(k, carry):
        dy = away(k)
        core_copy(dy).wait_recv()
        chip[dy] = part[c, lax.rem(y + dy, NY)] + given[dy]

        @pl.when(k > 0)
        def _():
            send_x(k - 1)

        return carry

    lax.fori_loop(0, NY, over_cores, 0)
    send_x(NY - 1)

    def send_y(k):
        dy = away(k)

        @pl.when(dy > 0)
        def _():
            y_copy(dy).start()

    def over_x(k, carry):
        dy = away(k)
        for dx in (1, 3, 2):
            x_copy(dx, dy).wait_recv()
        sum_x[dy] = chip[dy, x, :XROWS] + from_x[0, dy] + from_x[1, dy] + from_x[2, dy]

        @pl.when(k > 0)
        def _():
            send_y(k - 1)

        return carry

    lax.fori_loop(0, NY, over_x, 0)

    rest = chip[0, :, XROWS:]
    for dy in range(1, NY):
        u_copy(dy).wait_recv()
        rest = rest + last_y[dy]
    sum_y[...] = rest

    result = sum_x[0]
    for dy in range(1, NY):
        y_copy(dy).wait_recv()
        result = result + from_y[dy]
    total[:XROWS] = result
    for dx in (2, 1, 3):
        v_copy(dx).start()
    rest = sum_y[x]
    for dx in (1, 3, 2):
        v_copy(dx).wait_recv()
        rest = rest + last_x[dx - 1]
    total[XROWS:] = rest

    for low in range(NZL):
        tile = total[low * 8 : low * 8 + 8]
        for high in range(NZH):
            for core in range(NC):
                row = high * 4 + core * 2
                to_z[high * NZL + low, core] = tile[row : row + 2]

    def z_copy(dz, dc):
        core = lax.rem(c + dc, NC)
        return pltpu.make_async_remote_copy(
            src_ref=to_z.at[lax.rem(z + dz, NZ), core], dst_ref=from_z.at[dz, c],
            send_sem=z_send.at[dz, dc], recv_sem=z_recv.at[dz, dc],
            device_id=at(dz=dz, dc=dc), device_id_type=MESH,
        )

    from_z[0, c] = to_z[z, c]

    def start_z(k, carry):
        z_copy(k, 0).start()
        z_copy(k, 1).start()
        return carry

    lax.fori_loop(1, NZ, start_z, 0)
    z_copy(0, 1).start()

    loads[3].wait()
    for k in (1, 2, 3):
        block_copy(k).wait_recv()

    def tile_of(t, carry):
        left = jnp.concatenate([pool[slot_ref[t, b]] for b in range(8)], axis=1)
        right = weights[t].reshape(-1, weights.shape[-1])
        hidden_ref[0, t] = jnp.dot(left, right, preferred_element_type=jnp.float32).astype(jnp.bfloat16)
        return carry

    lax.fori_loop(0, 8, tile_of, 0)

    def wait_z(dz, dc):
        pltpu.make_async_remote_copy(
            src_ref=to_z.at[0, 0], dst_ref=from_z.at[dz, lax.rem(c + dc, NC)],
            send_sem=z_send.at[dz, dc], recv_sem=z_recv.at[dz, dc],
            device_id=at(dz=dz, dc=dc), device_id_type=MESH,
        ).wait_recv()

    def end_z(k, carry):
        wait_z(k, 0)
        wait_z(k, 1)
        return carry

    lax.fori_loop(1, NZ, end_z, 0)
    wait_z(0, 1)
    for core in range(NC):
        value = from_z[0, core]
        for dz in range(1, NZ):
            value = value + from_z[dz, core]
        grad_ref[:, core * half : (core + 1) * half] = value

    for k in (1, 2, 3):
        block_copy(k).wait_send()

    def drain_y(dy, carry):
        core_copy(dy).wait_send()
        for dx in (1, 2, 3):
            x_copy(dx, dy).wait_send()

        @pl.when(dy > 0)
        def _():
            y_copy(dy).wait_send()
            u_copy(dy).wait_send()

        return carry

    lax.fori_loop(0, NY, drain_y, 0)
    for dx in (1, 2, 3):
        v_copy(dx).wait_send()

    def drain_z(k, carry):
        z_copy(k, 0).wait_send()
        z_copy(k, 1).wait_send()
        return carry

    lax.fori_loop(1, NZ, drain_z, 0)
    z_copy(0, 1).wait_send()


def body(field, send_blocks, send_count, regrid_weights, tile_slot, edge_inputs, cotangent):
    tiles, reads, cells, nodes = regrid_weights.shape
    channels = field.shape[2]
    half = cotangent.shape[1] // 2
    f32, bf16 = jnp.float32, jnp.bfloat16
    dma = pltpu.SemaphoreType.DMA
    smem = pl.BlockSpec(memory_space=pltpu.SMEM)
    vmem = pl.BlockSpec(memory_space=pltpu.VMEM)
    hbm = pl.BlockSpec(memory_space=pl.ANY)
    return pl.pallas_call(
        kernel,
        name="regrid",
        out_shape=(
            jax.ShapeDtypeStruct((1, tiles, channels, nodes), bf16),
            jax.ShapeDtypeStruct((2, 2 * half), f32),
        ),
        in_specs=[smem, smem, smem, hbm, hbm, hbm, hbm],
        out_specs=(vmem, vmem),
        scratch_shapes=[
            pltpu.VMEM(field.shape[1:], bf16),
            pltpu.VMEM(regrid_weights.shape, bf16),
            pltpu.VMEM(edge_inputs.shape, bf16),
            pltpu.VMEM(cotangent.shape, bf16),
            pltpu.VMEM((3, 8, channels, cells), bf16),
            pltpu.VMEM((32, channels, cells), bf16),
            pltpu.VMEM((2, NY, NX, ROWS, half), f32),
            pltpu.VMEM((NY, NX, ROWS, half), f32),
            pltpu.VMEM((NY, NX, ROWS, half), f32),
            pltpu.VMEM((NX - 1, NY, XROWS, half), f32),
            pltpu.VMEM((NY, XROWS, half), f32),
            pltpu.VMEM((NY, XROWS, half), f32),
            pltpu.VMEM((NY, NX, ROWS - XROWS, half), f32),
            pltpu.VMEM((NX, ROWS - XROWS, half), f32),
            pltpu.VMEM((NX - 1, ROWS - XROWS, half), f32),
            pltpu.VMEM((ROWS, half), f32),
            pltpu.VMEM((NZ, NC, 2, half), f32),
            pltpu.VMEM((NZ, NC, 2, half), f32),
            dma((4,)),
            dma((3,)), dma((3,)),
            dma((NY,)), dma((NY,)),
            dma((NX - 1, NY)), dma((NX - 1, NY)),
            dma((NY,)), dma((NY,)),
            dma((NY,)), dma((NY,)),
            dma((NX - 1,)), dma((NX - 1,)),
            dma((NZ, NC)), dma((NZ, NC)),
        ],
        compiler_params=pltpu.CompilerParams(
            collective_id=0, has_side_effects=True, vmem_limit_bytes=56 * 2**20
        ),
    )(send_blocks, send_count, tile_slot, field, regrid_weights, edge_inputs, cotangent)


def solution(mesh):
    split = Mesh(mesh.devices.reshape(NY, NX, NZL, NZH, NC), AXES)
    rep, sp = AXES[:3], AXES[3:]
    return jax.shard_map(
        body,
        mesh=split,
        in_specs=(
            P(rep, sp, None, None),
            P(sp, None, None),
            P(sp, None),
            P(sp, None, None, None),
            P(sp, None),
            P(AXES, None),
            P(AXES, None),
        ),
        out_specs=(P(rep, sp, None, None), P(AXES, None)),
        check_vma=False,
    )
```

```python
import jax
import jax.numpy as jnp
from jax import lax
from jax.experimental import pallas as pl
from jax.experimental.pallas import tpu as pltpu
from jax.sharding import Mesh
from jax.sharding import PartitionSpec as P

AXES = ("y", "x", "zl", "zh", "c")
NY, NX, NZL, NZH, NC = 8, 4, 6, 2, 2
NZ = NZL * NZH
LANES = 128
ROWS = 96
FIRST = 80
MAIN = 96
PITCH = 40
XROWS = 72
MESH = pl.DeviceIdType.MESH


def kernel(
    blocks_hbm, count_hbm, slot_hbm, field_hbm, weights_hbm, edges_hbm, cot_hbm,
    hidden_ref, grad_ref,
    blocks_ref, count_ref, slot_ref, field, wide, weights, edges, cot,
    out_a, out_b, out_tail, pool_a, pool_b, pool_tail, tails, nodes,
    part, given, chip, from_x, sum_x, from_y, last_y, sum_y, last_x, total, to_z, from_z,
    in_sem, a_send, a_recv, d_send, d_recv, x_send, x_recv, y_send, y_recv,
    u_send, u_recv, v_send, v_recv, z_send, z_recv,
):
    y, x = lax.axis_index("y"), lax.axis_index("x")
    zl, zh, c = lax.axis_index("zl"), lax.axis_index("zh"), lax.axis_index("c")
    z = zh * NZL + zl
    own = zh * NC + c
    half = cot.shape[1] // 2

    def at(dy=0, dx=0, dz=0, dc=0):
        other = lax.rem(z + dz, NZ)
        return (
            lax.rem(y + dy, NY), lax.rem(x + dx, NX),
            lax.rem(other, NZL), lax.div(other, NZL), lax.rem(c + dc, NC),
        )

    loads = [
        pltpu.make_async_copy(source, goal, in_sem.at[k])
        for k, (source, goal) in enumerate(
            (
                (field_hbm, field), (edges_hbm, edges), (cot_hbm, cot), (weights_hbm, weights),
                (blocks_hbm, blocks_ref), (count_hbm, count_ref), (slot_hbm, slot_ref),
            )
        )
    ]

    barrier = pltpu.get_barrier_semaphore()

    def greet(**offset):
        pl.semaphore_signal(barrier, inc=1, device_id=at(**offset), device_id_type=MESH)

    for k in (6, 5, 7, 4, 8, 3, 9, 2, 10, 1, 11):
        greet(dz=k)
        greet(dz=k, dc=1)
        if k == 6:
            for load in loads:
                load.start()
    for k in (4, 3, 5, 2, 6, 1, 7):
        greet(dy=k)
    for k in (2, 1, 3):
        greet(dx=k)
    greet(dc=1)

    for k in (0, 4, 5):
        loads[k].wait()

    def widen(k, carry):
        for i in range(10):
            row = k * 10 + i
            wide[pl.ds(pl.multiple_of(row * PITCH, 8), 32)] = field[pl.ds(pl.multiple_of(row * 32, 32), 32)].astype(
                jnp.float32
            )
        return carry

    lax.fori_loop(0, 10, widen, 0)

    def gather(i, carry):
        k = lax.rem(i + 2, 4)
        shard = lax.rem(zh + lax.div(k, 2), NZH) * NC + lax.rem(c + lax.rem(k, 2), NC)
        last = []
        for j in range(8):
            start = blocks_ref[0, shard, j]
            alive = j < count_ref[0, shard]
            main = wide[pl.ds(start, MAIN, stride=PITCH)]
            main = jnp.where(alive, main, jnp.zeros_like(main)).astype(jnp.bfloat16)
            out_a[k, j] = main[:FIRST]
            out_b[k, j] = main[FIRST:]
            tail = wide[pl.ds(start + MAIN * PITCH, 4, stride=PITCH)]
            last.append(jnp.where(alive, tail, jnp.zeros_like(tail)))
        out_tail[k] = jnp.concatenate(last, axis=0).astype(jnp.bfloat16)
        return carry

    lax.fori_loop(0, 4, gather, 0)
    pool_a[pl.ds(own * 8, 8)] = out_a[0]
    pool_b[pl.ds(own * 8, 8)] = out_b[0]
    pool_tail[own] = out_tail[0]

    loads[1].wait()
    loads[2].wait()
    for k in range(4):
        piece = lax.dot_general(
            edges[:, k * 384 : (k + 1) * 384], cot[...], (((0,), (0,)), ((), ())),
            preferred_element_type=jnp.float32,
        )
        for h in range(2):
            for g in range(2):
                column = h * half + g * LANES
                part[h, 2 * k : 2 * k + 2, :, g * 48 : g * 48 + 48] = piece[:, column : column + LANES].reshape(
                    2, NX, 48, LANES
                )

    pl.semaphore_wait(barrier, 2 * (NZ - 1) + (NY - 1) + (NX - 1) + 1)

    def remote(source, goal, send, recv, **offset):
        return pltpu.make_async_remote_copy(
            src_ref=source, dst_ref=goal, send_sem=send, recv_sem=recv,
            device_id=at(**offset), device_id_type=MESH,
        )

    def block_copy(k, kind):
        source, goal = (
            (out_a.at[k], pool_a.at[pl.ds(own * 8, 8)]),
            (out_tail.at[k], pool_tail.at[own]),
            (out_b.at[k], pool_b.at[pl.ds(own * 8, 8)]),
        )[kind]
        return remote(source, goal, a_send.at[kind], a_recv.at[kind], dz=NZL * (k // 2), dc=k % 2)

    def all_blocks(kind):
        whole = (pool_a.at[pl.ds(0, 24)], pool_tail.at[pl.ds(0, 3)], pool_b.at[pl.ds(0, 24)])[kind]
        return remote(whole, whole, a_send.at[kind], a_recv.at[kind], dc=1)

    for k in (2, 3):
        for kind in (0, 1):
            block_copy(k, kind).start()
    for kind in range(3):
        block_copy(1, kind).start()

    def away(k):
        return 4 + lax.div(k, 2) * (1 - 2 * lax.rem(k, 2)) - lax.rem(k, 2)

    def core_copy(dy):
        return remote(
            part.at[1 - c, lax.rem(y + dy, NY)], given.at[dy], d_send.at[0], d_recv.at[dy], dc=1
        )

    def x_copy(dx, dy):
        return remote(
            chip.at[dy, lax.rem(x + dx, NX), pl.ds(0, XROWS)], from_x.at[dy, dx - 1],
            x_send.at[0], x_recv.at[dy], dx=dx,
        )

    def y_copy(dy):
        return remote(sum_x.at[dy], from_y.at[dy], y_send.at[0], y_recv.at[0], dy=dy)

    def u_copy(dy):
        return remote(
            chip.at[dy, :, pl.ds(XROWS, ROWS - XROWS)], last_y.at[dy], u_send.at[0], u_recv.at[0], dy=dy
        )

    def v_copy(dx):
        return remote(sum_y.at[lax.rem(x + dx, NX)], last_x.at[dx - 1], v_send.at[0], v_recv.at[0], dx=dx)

    def all_of(whole, send, recv):
        return remote(whole, whole, send, recv, dc=1)

    all_x = all_of(from_x, x_send.at[0], x_recv.at[0])
    all_y = all_of(from_y.at[pl.ds(1, NY - 1)], y_send.at[0], y_recv.at[0])
    all_u = all_of(last_y.at[pl.ds(1, NY - 1)], u_send.at[0], u_recv.at[0])
    all_v = all_of(last_x, v_send.at[0], v_recv.at[0])

    def start_core(k, carry):
        core_copy(away(k)).start()
        return carry

    lax.fori_loop(0, NY, start_core, 0)

    def send_x(k):
        dy = away(k)
        for dx in (2, 1, 3):
            x_copy(dx, dy).start()

        @pl.when(dy > 0)
        def _():
            u_copy(dy).start()

    def over_cores(k, carry):
        dy = away(k)
        core_copy(dy).wait_recv()
        chip[dy] = part[c, lax.rem(y + dy, NY)] + given[dy]

        @pl.when(k > 0)
        def _():
            send_x(k - 1)

        return carry

    lax.fori_loop(0, NY, over_cores, 0)
    send_x(NY - 1)

    def send_y(k):
        dy = away(k)

        @pl.when(dy > 0)
        def _():
            y_copy(dy).start()

    def over_x(k, carry):
        dy = away(k)
        all_of(from_x.at[dy], x_send.at[0], x_recv.at[dy]).wait_recv()
        sum_x[dy] = chip[dy, x, :XROWS] + from_x[dy, 0] + from_x[dy, 1] + from_x[dy, 2]

        @pl.when(k > 0)
        def _():
            send_y(k - 1)

        return carry

    lax.fori_loop(0, NY, over_x, 0)

    rest = chip[0, :, XROWS:]
    all_u.wait_recv()
    for dy in range(1, NY):
        rest = rest + last_y[dy]
    sum_y[...] = rest

    result = sum_x[0]
    for dx in (2, 1, 3):
        v_copy(dx).start()
    all_y.wait_recv()
    for dy in range(1, NY):
        result = result + from_y[dy]
    total[:XROWS] = result
    rest = sum_y[x]
    all_v.wait_recv()
    for dx in range(1, NX):
        rest = rest + last_x[dx - 1]
    total[XROWS:] = rest

    for low in range(NZL):
        for group in range(2):
            tile = total[group * 48 + low * 8 : group * 48 + low * 8 + 8]
            for high in range(NZH):
                for core in range(NC):
                    row = high * 4 + core * 2
                    to_z[(high * NZL + low) * NC + core, :, group * LANES : (group + 1) * LANES] = tile[row : row + 2]

    def z_copy(dz, dc):
        return remote(
            to_z.at[lax.rem(z + dz, NZ) * NC + lax.rem(c + dc, NC)], from_z.at[dz * NC + c],
            z_send.at[0], z_recv.at[0], dz=dz, dc=dc,
        )

    all_z = all_of(from_z.at[pl.ds(0, NZ * NC - 1)], z_send.at[0], z_recv.at[0])
    from_z[c] = to_z[z * NC + c]

    def start_z(k, carry):
        z_copy(k, 0).start()
        z_copy(k, 1).start()
        return carry

    lax.fori_loop(1, NZ, start_z, 0)
    z_copy(0, 1).start()

    for k in (2, 3):
        block_copy(k, 2).start()

    loads[3].wait()
    loads[6].wait()
    for kind in (0, 1):
        all_blocks(kind).wait_recv()
    for shard in range(NZH * NC):
        rows = pool_tail[shard].astype(jnp.float32)
        for j in range(8):
            tails[shard * 8 + j] = jnp.concatenate([rows[4 * j : 4 * j + 4]] * 4, axis=0)

    def first_channels(t, carry):
        def rows(b):
            last = tails[slot_ref[t, b]].astype(jnp.bfloat16)
            return jnp.concatenate([pool_a[slot_ref[t, b]], last], axis=0)

        left = jnp.concatenate([rows(b) for b in range(8)], axis=1)
        right = weights[t].reshape(-1, weights.shape[-1])
        value = jnp.dot(left, right, preferred_element_type=jnp.float32)
        nodes[pl.ds(t, FIRST, stride=8)] = value[:FIRST]
        nodes[pl.ds(MAIN * 8 + t, 4, stride=8)] = value[FIRST : FIRST + 4]
        return carry

    lax.fori_loop(0, 8, first_channels, 0, unroll=True)
    hidden_ref[: FIRST * 8] = nodes[: FIRST * 8].astype(jnp.bfloat16)
    hidden_ref[MAIN * 8 :] = nodes[MAIN * 8 :].astype(jnp.bfloat16)

    all_z.wait_recv()
    for core in range(NC):
        value = from_z[core]
        for dz in range(1, NZ):
            value = value + from_z[dz * NC + core]
        grad_ref[:, core * half : (core + 1) * half] = value

    all_blocks(2).wait_recv()

    def other_channels(t, carry):
        left = jnp.concatenate([pool_b[slot_ref[t, b]] for b in range(8)], axis=1)
        right = weights[t].reshape(-1, weights.shape[-1])
        nodes[pl.ds(FIRST * 8 + t, MAIN - FIRST, stride=8)] = jnp.dot(
            left, right, preferred_element_type=jnp.float32
        )
        return carry

    lax.fori_loop(0, 8, other_channels, 0, unroll=True)
    hidden_ref[FIRST * 8 : MAIN * 8] = nodes[FIRST * 8 : MAIN * 8].astype(jnp.bfloat16)

    for kind in range(3):
        all_blocks(kind).wait_send()
    all_of(given, d_send.at[0], d_recv.at[0]).wait_send()
    for copies in (all_x, all_y, all_u, all_v, all_z):
        copies.wait_send()


def body(field, send_blocks, send_count, regrid_weights, tile_slot, edge_inputs, cotangent):
    tiles, reads, cells, nodes = regrid_weights.shape
    blocks, channels = field.shape[1:3]
    half = cotangent.shape[1] // 2
    field = jnp.transpose(field, (0, 2, 1, 3)).reshape(channels * blocks, cells)
    f32, bf16 = jnp.float32, jnp.bfloat16
    dma = pltpu.SemaphoreType.DMA
    vmem = pl.BlockSpec(memory_space=pltpu.VMEM)
    hbm = pl.BlockSpec(memory_space=pl.ANY)
    hidden, grad = pl.pallas_call(
        kernel,
        name="regrid",
        out_shape=(
            pltpu.VMEM((channels * tiles, nodes), bf16),
            pltpu.VMEM((2, 2 * half), f32),
        ),
        in_specs=[hbm] * 7,
        out_specs=(vmem, vmem),
        scratch_shapes=[
            pltpu.SMEM(send_blocks.shape, jnp.int32),
            pltpu.SMEM(send_count.shape, jnp.int32),
            pltpu.SMEM(tile_slot.shape, jnp.int32),
            pltpu.VMEM(field.shape, bf16),
            pltpu.VMEM((channels * PITCH, cells), f32),
            pltpu.VMEM(regrid_weights.shape, bf16),
            pltpu.VMEM(edge_inputs.shape, bf16),
            pltpu.VMEM(cotangent.shape, bf16),
            pltpu.VMEM((4, 8, FIRST, cells), bf16),
            pltpu.VMEM((4, 8, MAIN - FIRST, cells), bf16),
            pltpu.VMEM((4, 32, cells), bf16),
            pltpu.VMEM((32, FIRST, cells), bf16),
            pltpu.VMEM((32, MAIN - FIRST, cells), bf16),
            pltpu.VMEM((4, 32, cells), bf16),
            pltpu.VMEM((32, 16, cells), f32),
            pltpu.VMEM((channels * tiles, nodes), f32),
            pltpu.VMEM((2, NY, NX, ROWS, LANES), f32),
            pltpu.VMEM((NY, NX, ROWS, LANES), f32),
            pltpu.VMEM((NY, NX, ROWS, LANES), f32),
            pltpu.VMEM((NY, NX - 1, XROWS, LANES), f32),
            pltpu.VMEM((NY, XROWS, LANES), f32),
            pltpu.VMEM((NY, XROWS, LANES), f32),
            pltpu.VMEM((NY, NX, ROWS - XROWS, LANES), f32),
            pltpu.VMEM((NX, ROWS - XROWS, LANES), f32),
            pltpu.VMEM((NX - 1, ROWS - XROWS, LANES), f32),
            pltpu.VMEM((ROWS, LANES), f32),
            pltpu.VMEM((NZ * NC, 2, half), f32),
            pltpu.VMEM((NZ * NC, 2, half), f32),
            dma((7,)),
            dma((3,)), dma((3,)),
            dma((1,)), dma((NY,)),
            dma((1,)), dma((NY,)),
            dma((1,)), dma((1,)),
            dma((1,)), dma((1,)),
            dma((1,)), dma((1,)),
            dma((1,)), dma((1,)),
        ],
        compiler_params=pltpu.CompilerParams(
            collective_id=0, has_side_effects=True, vmem_limit_bytes=56 * 2**20
        ),
    )(send_blocks, send_count, tile_slot, field, regrid_weights, edge_inputs, cotangent)
    return jnp.transpose(hidden.reshape(1, channels, tiles, nodes), (0, 2, 1, 3)), grad


def solution(mesh):
    split = Mesh(mesh.devices.reshape(NY, NX, NZL, NZH, NC), AXES)
    rep, sp = AXES[:3], AXES[3:]
    return jax.shard_map(
        body,
        mesh=split,
        in_specs=(
            P(rep, sp, None, None),
            P(sp, None, None),
            P(sp, None),
            P(sp, None, None, None),
            P(sp, None),
            P(AXES, None),
            P(AXES, None),
        ),
        out_specs=(P(rep, sp, None, None), P(AXES, None)),
        check_vma=False,
    )
```

```python
import jax
import jax.numpy as jnp
from jax import lax
from jax.experimental import pallas as pl
from jax.experimental.pallas import tpu as pltpu
from jax.sharding import Mesh
from jax.sharding import PartitionSpec as P

AXES = ("y", "x", "zl", "zh", "c")
NY, NX, NZL, NZH, NC = 8, 4, 6, 2, 2
NZ = NZL * NZH
LANES = 128
ROWS = 96
FIRST = 64
LATER = 16
MAIN = 96
PITCH = 40
XROWS = 72
MESH = pl.DeviceIdType.MESH


def kernel(
    blocks_hbm, count_hbm, slot_hbm, field_hbm, weights_hbm, edges_hbm, cot_hbm,
    hidden_ref, grad_ref,
    blocks_ref, count_ref, slot_ref, field, wide, weights, edges, cot,
    out_a, out_b, out_tail, pool_a, pool_b, pool_c, pool_tail, tails, nodes,
    part, given, chip, from_x, sum_x, from_y, last_y, sum_y, last_x, total, to_z, from_z,
    near, far, in_sem, a_send, a_recv, d_send, d_recv, x_send, x_recv, y_send, y_recv,
    u_send, u_recv, v_send, v_recv, z_send, z_recv,
):
    y, x = lax.axis_index("y"), lax.axis_index("x")
    zl, zh, c = lax.axis_index("zl"), lax.axis_index("zh"), lax.axis_index("c")
    z = zh * NZL + zl
    own = zh * NC + c
    half = cot.shape[1] // 2

    def at(dy=0, dx=0, dz=0, dc=0):
        other = lax.rem(z + dz, NZ)
        return (
            lax.rem(y + dy, NY), lax.rem(x + dx, NX),
            lax.rem(other, NZL), lax.div(other, NZL), lax.rem(c + dc, NC),
        )

    loads = [
        pltpu.make_async_copy(source, goal, in_sem.at[k])
        for k, (source, goal) in enumerate(
            (
                (field_hbm, field), (edges_hbm, edges), (cot_hbm, cot), (weights_hbm, weights),
                (blocks_hbm, blocks_ref), (count_hbm, count_ref), (slot_hbm, slot_ref),
            )
        )
    ]

    barrier = pltpu.get_barrier_semaphore()

    def greet(**offset):
        pl.semaphore_signal(barrier, inc=1, device_id=at(**offset), device_id_type=MESH)

    greet(dz=NZL)
    greet(dz=NZL, dc=1)
    for load in loads:
        load.start()
    for k in (1, NZ - 1):
        greet(dz=k)
        greet(dz=k, dc=1)
    for k in (1, NY - 1):
        greet(dy=k)
    for k in (1, NX - 1):
        greet(dx=k)
    greet(dc=1)

    for k in (0, 4, 5):
        loads[k].wait()

    def widen(k, carry):
        for i in range(10):
            row = k * 10 + i
            wide[pl.ds(pl.multiple_of(row * PITCH, 8), 32)] = field[pl.ds(pl.multiple_of(row * 32, 32), 32)].astype(
                jnp.float32
            )
        return carry

    lax.fori_loop(0, 10, widen, 0)

    def gather(i, carry):
        k = lax.rem(i + 2, 4)
        shard = lax.rem(zh + lax.div(k, 2), NZH) * NC + lax.rem(c + lax.rem(k, 2), NC)
        last = []
        for j in range(8):
            start = blocks_ref[0, shard, j]
            alive = j < count_ref[0, shard]
            main = wide[pl.ds(start, MAIN, stride=PITCH)]
            main = jnp.where(alive, main, jnp.zeros_like(main)).astype(jnp.bfloat16)
            out_a[k, j] = main[:FIRST]
            out_b[0, k, j] = main[FIRST : FIRST + LATER]
            out_b[1, k, j] = main[FIRST + LATER :]
            tail = wide[pl.ds(start + MAIN * PITCH, 4, stride=PITCH)]
            last.append(jnp.where(alive, tail, jnp.zeros_like(tail)))
        out_tail[k] = jnp.concatenate(last, axis=0).astype(jnp.bfloat16)
        return carry

    lax.fori_loop(0, 4, gather, 0)
    pool_a[pl.ds(own * 8, 8)] = out_a[0]
    for later in range(2):
        (pool_b, pool_c)[later][pl.ds(own * 8, 8)] = out_b[later, 0]
    pool_tail[own] = out_tail[0]

    def own_gradient():
        loads[1].wait()
        loads[2].wait()
        for k in range(4):
            piece = lax.dot_general(
                edges[:, k * 384 : (k + 1) * 384], cot[...], (((0,), (0,)), ((), ())),
                preferred_element_type=jnp.float32,
            )
            for h in range(2):
                for g in range(2):
                    column = h * half + g * LANES
                    part[h, 2 * k : 2 * k + 2, :, g * 48 : g * 48 + 48] = piece[:, column : column + LANES].reshape(
                        2, NX, 48, LANES
                    )

    @pl.when(zh == 0)
    def _():
        own_gradient()

    pl.semaphore_wait(barrier, 11)

    def tell_xy(r):
        first = (dict(dy=1), dict(dy=NY - 1), dict(dx=1), dict(dx=NX - 1))
        second = (dict(dy=1), dict(dy=NY - 1), dict(dy=2), dict(dy=NY - 2))
        for offset in (first, second)[r]:
            pl.semaphore_signal(near.at[r], inc=1, device_id=at(**offset), device_id_type=MESH)

    def tell_z(r):
        for k in (NZL, 1, NZ - 1):
            pl.semaphore_signal(far.at[r], inc=1, device_id=at(dz=k), device_id_type=MESH)


    def remote(source, goal, send, recv, **offset):
        return pltpu.make_async_remote_copy(
            src_ref=source, dst_ref=goal, send_sem=send, recv_sem=recv,
            device_id=at(**offset), device_id_type=MESH,
        )

    def block_copy(k, kind):
        source, goal = (
            (out_a.at[k], pool_a.at[pl.ds(own * 8, 8)]),
            (out_tail.at[k], pool_tail.at[own]),
            (out_b.at[0, k], pool_b.at[pl.ds(own * 8, 8)]),
            (out_b.at[1, k], pool_c.at[pl.ds(own * 8, 8)]),
        )[kind]
        return remote(source, goal, a_send.at[kind], a_recv.at[kind], dz=NZL * (k // 2), dc=k % 2)

    def all_blocks(kind):
        whole = (
            pool_a.at[pl.ds(0, 24)], pool_tail.at[pl.ds(0, 3)],
            pool_b.at[pl.ds(0, 24)], pool_c.at[pl.ds(0, 24)],
        )[kind]
        return remote(whole, whole, a_send.at[kind], a_recv.at[kind], dc=1)

    for k in (2, 3):
        for kind in (0, 1):
            block_copy(k, kind).start()

    @pl.when(zh == 1)
    def _():
        for k in (2, 3):
            block_copy(k, 2).start()

    for kind in range(4):
        block_copy(1, kind).start()

    tell_xy(0)

    @pl.when(zh == 1)
    def _():
        own_gradient()

    def away(k):
        return 4 + lax.div(k, 2) * (1 - 2 * lax.rem(k, 2)) - lax.rem(k, 2)

    def core_copy(dy):
        return remote(
            part.at[1 - c, lax.rem(y + dy, NY)], given.at[dy], d_send.at[0], d_recv.at[dy], dc=1
        )

    def x_copy(dx, dy):
        return remote(
            chip.at[dy, lax.rem(x + dx, NX), pl.ds(0, XROWS)], from_x.at[dy, dx - 1],
            x_send.at[0], x_recv.at[dy], dx=dx,
        )

    def y_copy(dy):
        return remote(sum_x.at[dy], from_y.at[dy], y_send.at[0], y_recv.at[0], dy=dy)

    def u_copy(dy):
        return remote(
            chip.at[dy, :, pl.ds(XROWS, ROWS - XROWS)], last_y.at[dy], u_send.at[0], u_recv.at[0], dy=dy
        )

    def v_copy(dx):
        return remote(sum_y.at[lax.rem(x + dx, NX)], last_x.at[dx - 1], v_send.at[0], v_recv.at[0], dx=dx)

    def all_of(whole, send, recv):
        return remote(whole, whole, send, recv, dc=1)

    all_x = all_of(from_x, x_send.at[0], x_recv.at[0])
    all_y = all_of(from_y.at[pl.ds(1, NY - 1)], y_send.at[0], y_recv.at[0])
    all_u = all_of(last_y.at[pl.ds(1, NY - 1)], u_send.at[0], u_recv.at[0])
    all_v = all_of(last_x, v_send.at[0], v_recv.at[0])

    def start_core(k, carry):
        core_copy(away(k)).start()
        return carry

    lax.fori_loop(0, NY, start_core, 0)
    tell_z(0)

    def send_x(k):
        dy = away(k)
        for dx in (2, 1, 3):
            x_copy(dx, dy).start()

    def over_cores(k, carry):
        dy = away(k)
        core_copy(dy).wait_recv()
        chip[dy] = part[c, lax.rem(y + dy, NY)] + given[dy]

        @pl.when(k == 0)
        def _():
            pl.semaphore_wait(near.at[0], 4)
            tell_xy(1)

        @pl.when(k > 0)
        def _():
            send_x(k - 1)

        @pl.when(k == 2)
        def _():
            pl.semaphore_wait(near.at[1], 4)

        @pl.when((k == 3) | (k == 4))
        def _():
            u_copy(away(2 * k - 6)).start()
            u_copy(away(2 * k - 5)).start()

        @pl.when(k > 4)
        def _():
            u_copy(away(k - 1)).start()

        return carry

    lax.fori_loop(0, NY, over_cores, 0)
    send_x(NY - 1)

    def send_y(k):
        dy = away(k)

        @pl.when(dy > 0)
        def _():
            y_copy(dy).start()

    def over_x(k, carry):
        dy = away(k)
        all_of(from_x.at[dy], x_send.at[0], x_recv.at[dy]).wait_recv()
        sum_x[dy] = chip[dy, x, :XROWS] + from_x[dy, 0] + from_x[dy, 1] + from_x[dy, 2]

        @pl.when(k > 0)
        def _():
            send_y(k - 1)

        @pl.when(k == 3)
        def _():
            pl.semaphore_wait(far.at[0], 3)
            tell_z(1)

        return carry

    lax.fori_loop(0, NY, over_x, 0)

    rest = chip[0, :, XROWS:]
    all_u.wait_recv()
    for dy in range(1, NY):
        rest = rest + last_y[dy]
    sum_y[...] = rest

    result = sum_x[0]
    for dx in (2, 1, 3):
        v_copy(dx).start()
    all_y.wait_recv()
    for dy in range(1, NY):
        result = result + from_y[dy]
    total[:XROWS] = result
    rest = sum_y[x]
    all_v.wait_recv()
    for dx in range(1, NX):
        rest = rest + last_x[dx - 1]
    total[XROWS:] = rest

    for low in range(NZL):
        for group in range(2):
            tile = total[group * 48 + low * 8 : group * 48 + low * 8 + 8]
            for high in range(NZH):
                for core in range(NC):
                    row = high * 4 + core * 2
                    to_z[(high * NZL + low) * NC + core, :, group * LANES : (group + 1) * LANES] = tile[row : row + 2]

    def z_copy(dz, dc):
        return remote(
            to_z.at[lax.rem(z + dz, NZ) * NC + lax.rem(c + dc, NC)], from_z.at[dz * NC + c],
            z_send.at[0], z_recv.at[0], dz=dz, dc=dc,
        )

    all_z = all_of(from_z.at[pl.ds(0, NZ * NC - 1)], z_send.at[0], z_recv.at[0])
    from_z[c] = to_z[z * NC + c]

    pl.semaphore_wait(far.at[1], 3)

    def start_z(k, carry):
        z_copy(k, 0).start()
        z_copy(k, 1).start()
        return carry

    lax.fori_loop(1, NZ, start_z, 0)
    z_copy(0, 1).start()

    @pl.when(zh == 0)
    def _():
        for k in (2, 3):
            block_copy(k, 2).start()

    for k in (2, 3):
        block_copy(k, 3).start()

    loads[3].wait()
    loads[6].wait()
    for kind in (0, 1):
        all_blocks(kind).wait_recv()
    for shard in range(NZH * NC):
        rows = pool_tail[shard].astype(jnp.float32)
        for j in range(8):
            tails[shard * 8 + j] = jnp.concatenate([rows[4 * j : 4 * j + 4]] * 4, axis=0)

    def first_channels(t, carry):
        def rows(b):
            last = tails[slot_ref[t, b]].astype(jnp.bfloat16)
            return jnp.concatenate([pool_a[slot_ref[t, b]], last], axis=0)

        left = jnp.concatenate([rows(b) for b in range(8)], axis=1)
        right = weights[t].reshape(-1, weights.shape[-1])
        value = jnp.dot(left, right, preferred_element_type=jnp.float32)
        nodes[pl.ds(t, FIRST, stride=8)] = value[:FIRST]
        nodes[pl.ds(MAIN * 8 + t, 4, stride=8)] = value[FIRST : FIRST + 4]
        return carry

    lax.fori_loop(0, 8, first_channels, 0, unroll=True)
    hidden_ref[: FIRST * 8] = nodes[: FIRST * 8].astype(jnp.bfloat16)
    hidden_ref[MAIN * 8 :] = nodes[MAIN * 8 :].astype(jnp.bfloat16)

    def other_channels(p):
        all_blocks(2 + p).wait_recv()
        start = FIRST + p * LATER
        pool = (pool_b, pool_c)[p]
        for t in range(8):
            left = jnp.concatenate([pool[slot_ref[t, b]] for b in range(8)], axis=1)
            right = weights[t].reshape(-1, weights.shape[-1])
            nodes[pl.ds(start * 8 + t, LATER, stride=8)] = jnp.dot(left, right, preferred_element_type=jnp.float32)
        rows = slice(start * 8, (start + LATER) * 8)
        hidden_ref[rows] = nodes[rows].astype(jnp.bfloat16)

    other_channels(0)

    all_z.wait_recv()
    for core in range(NC):
        value = from_z[core]
        for dz in range(1, NZ):
            value = value + from_z[dz * NC + core]
        grad_ref[:, core * half : (core + 1) * half] = value

    other_channels(1)

    for kind in range(4):
        all_blocks(kind).wait_send()
    all_of(given, d_send.at[0], d_recv.at[0]).wait_send()
    for copies in (all_x, all_y, all_u, all_v, all_z):
        copies.wait_send()


def body(field, send_blocks, send_count, regrid_weights, tile_slot, edge_inputs, cotangent):
    tiles, reads, cells, nodes = regrid_weights.shape
    blocks, channels = field.shape[1:3]
    half = cotangent.shape[1] // 2
    field = jnp.transpose(field, (0, 2, 1, 3)).reshape(channels * blocks, cells)
    f32, bf16 = jnp.float32, jnp.bfloat16
    dma = pltpu.SemaphoreType.DMA
    vmem = pl.BlockSpec(memory_space=pltpu.VMEM)
    hbm = pl.BlockSpec(memory_space=pl.ANY)
    hidden, grad = pl.pallas_call(
        kernel,
        name="regrid",
        out_shape=(
            pltpu.VMEM((channels * tiles, nodes), bf16),
            pltpu.VMEM((2, 2 * half), f32),
        ),
        in_specs=[hbm] * 7,
        out_specs=(vmem, vmem),
        scratch_shapes=[
            pltpu.SMEM(send_blocks.shape, jnp.int32),
            pltpu.SMEM(send_count.shape, jnp.int32),
            pltpu.SMEM(tile_slot.shape, jnp.int32),
            pltpu.VMEM(field.shape, bf16),
            pltpu.VMEM((channels * PITCH, cells), f32),
            pltpu.VMEM(regrid_weights.shape, bf16),
            pltpu.VMEM(edge_inputs.shape, bf16),
            pltpu.VMEM(cotangent.shape, bf16),
            pltpu.VMEM((4, 8, FIRST, cells), bf16),
            pltpu.VMEM((2, 4, 8, LATER, cells), bf16),
            pltpu.VMEM((4, 32, cells), bf16),
            pltpu.VMEM((32, FIRST, cells), bf16),
            pltpu.VMEM((32, LATER, cells), bf16),
            pltpu.VMEM((32, LATER, cells), bf16),
            pltpu.VMEM((4, 32, cells), bf16),
            pltpu.VMEM((32, 16, cells), f32),
            pltpu.VMEM((channels * tiles, nodes), f32),
            pltpu.VMEM((2, NY, NX, ROWS, LANES), f32),
            pltpu.VMEM((NY, NX, ROWS, LANES), f32),
            pltpu.VMEM((NY, NX, ROWS, LANES), f32),
            pltpu.VMEM((NY, NX - 1, XROWS, LANES), f32),
            pltpu.VMEM((NY, XROWS, LANES), f32),
            pltpu.VMEM((NY, XROWS, LANES), f32),
            pltpu.VMEM((NY, NX, ROWS - XROWS, LANES), f32),
            pltpu.VMEM((NX, ROWS - XROWS, LANES), f32),
            pltpu.VMEM((NX - 1, ROWS - XROWS, LANES), f32),
            pltpu.VMEM((ROWS, LANES), f32),
            pltpu.VMEM((NZ * NC, 2, half), f32),
            pltpu.VMEM((NZ * NC, 2, half), f32),
            pltpu.SemaphoreType.REGULAR((2,)),
            pltpu.SemaphoreType.REGULAR((2,)),
            dma((7,)),
            dma((4,)), dma((4,)),
            dma((1,)), dma((NY,)),
            dma((1,)), dma((NY,)),
            dma((1,)), dma((1,)),
            dma((1,)), dma((1,)),
            dma((1,)), dma((1,)),
            dma((1,)), dma((1,)),
        ],
        compiler_params=pltpu.CompilerParams(
            collective_id=0, has_side_effects=True, vmem_limit_bytes=56 * 2**20
        ),
    )(send_blocks, send_count, tile_slot, field, regrid_weights, edge_inputs, cotangent)
    return jnp.transpose(hidden.reshape(1, channels, tiles, nodes), (0, 2, 1, 3)), grad


def solution(mesh):
    split = Mesh(mesh.devices.reshape(NY, NX, NZL, NZH, NC), AXES)
    rep, sp = AXES[:3], AXES[3:]
    return jax.shard_map(
        body,
        mesh=split,
        in_specs=(
            P(rep, sp, None, None),
            P(sp, None, None),
            P(sp, None),
            P(sp, None, None, None),
            P(sp, None),
            P(AXES, None),
            P(AXES, None),
        ),
        out_specs=(P(rep, sp, None, None), P(AXES, None)),
        check_vma=False,
    )
```

```python
import jax
import jax.numpy as jnp
from jax import lax
from jax.experimental import pallas as pl
from jax.experimental.pallas import tpu as pltpu
from jax.sharding import Mesh
from jax.sharding import PartitionSpec as P

AXES = ("y", "x", "zl", "zh", "c")
NY, NX, NZL, NZH, NC = 8, 4, 6, 2, 2
NZ = NZL * NZH
LANES = 128
ROWS = 96
FIRST, SECOND, THIRD = 64, 16, 16
MAIN = FIRST + SECOND + THIRD
PITCH = 40
XROWS = 72
MESH = pl.DeviceIdType.MESH


def kernel(
    blocks_hbm, count_hbm, slot_hbm, field_hbm, weights_hbm, edges_hbm, cot_hbm,
    hidden_ref, grad_ref,
    blocks_ref, count_ref, slot_ref, field, wide, weights, edges, cot,
    out_a, out_b, out_c, out_tail, pool_a, pool_b, pool_c, pool_tail, tails, nodes,
    part, given, chip, from_x, sum_x, from_y, last_y, sum_y, last_x, total, to_z, from_z, to_core, from_core,
    near, far, in_sem, a_send, a_recv, d_send, d_recv, x_send, x_recv, y_send, y_recv,
    u_send, u_recv, v_send, v_recv, z_send, z_recv,
):
    y, x = lax.axis_index("y"), lax.axis_index("x")
    zl, zh, c = lax.axis_index("zl"), lax.axis_index("zh"), lax.axis_index("c")
    z = zh * NZL + zl
    own = zh * NC + c
    half = cot.shape[1] // 2

    def at(dy=0, dx=0, dz=0, dc=0):
        other = lax.rem(z + dz, NZ)
        return (
            lax.rem(y + dy, NY), lax.rem(x + dx, NX),
            lax.rem(other, NZL), lax.div(other, NZL), lax.rem(c + dc, NC),
        )

    loads = [
        pltpu.make_async_copy(source, goal, in_sem.at[k])
        for k, (source, goal) in enumerate(
            (
                (field_hbm, field), (edges_hbm, edges), (cot_hbm, cot), (weights_hbm, weights),
                (blocks_hbm, blocks_ref), (count_hbm, count_ref), (slot_hbm, slot_ref),
            )
        )
    ]

    barrier = pltpu.get_barrier_semaphore()

    def greet(**offset):
        pl.semaphore_signal(barrier, inc=1, device_id=at(**offset), device_id_type=MESH)

    greet(dz=NZL)
    greet(dz=NZL, dc=1)
    for load in loads:
        load.start()
    for k in (1, NZ - 1):
        greet(dz=k)
        greet(dz=k, dc=1)
    for k in (1, NY - 1):
        greet(dy=k)
    for k in (1, NX - 1):
        greet(dx=k)
    greet(dc=1)

    for k in (0, 4, 5):
        loads[k].wait()

    def widen(k, carry):
        for i in range(10):
            row = k * 10 + i
            wide[pl.ds(pl.multiple_of(row * PITCH, 8), 32)] = field[pl.ds(pl.multiple_of(row * 32, 32), 32)].astype(
                jnp.float32
            )
        return carry

    lax.fori_loop(0, 10, widen, 0)

    def gather(i, carry):
        k = lax.rem(i + 2, 4)
        shard = lax.rem(zh + lax.div(k, 2), NZH) * NC + lax.rem(c + lax.rem(k, 2), NC)
        last = []
        for j in range(8):
            start = blocks_ref[0, shard, j]
            alive = j < count_ref[0, shard]
            main = wide[pl.ds(start, MAIN, stride=PITCH)]
            main = jnp.where(alive, main, jnp.zeros_like(main)).astype(jnp.bfloat16)
            out_a[k, j] = main[:FIRST]
            out_b[k, j] = main[FIRST : FIRST + SECOND]
            out_c[k, j] = main[FIRST + SECOND :]
            tail = wide[pl.ds(start + MAIN * PITCH, 4, stride=PITCH)]
            last.append(jnp.where(alive, tail, jnp.zeros_like(tail)))
        out_tail[k] = jnp.concatenate(last, axis=0).astype(jnp.bfloat16)
        return carry

    lax.fori_loop(0, 4, gather, 0)
    pool_a[pl.ds(own * 8, 8)] = out_a[0]
    pool_b[pl.ds(own * 8, 8)] = out_b[0]
    pool_c[pl.ds(own * 8, 8)] = out_c[0]
    pool_tail[own] = out_tail[0]

    def own_gradient():
        loads[1].wait()
        loads[2].wait()
        for k in range(4):
            piece = lax.dot_general(
                edges[:, k * 384 : (k + 1) * 384], cot[...], (((0,), (0,)), ((), ())),
                preferred_element_type=jnp.float32,
            )
            for h in range(2):
                for g in range(2):
                    column = h * half + g * LANES
                    part[h, 2 * k : 2 * k + 2, :, g * 48 : g * 48 + 48] = piece[:, column : column + LANES].reshape(
                        2, NX, 48, LANES
                    )

    @pl.when(zh == 0)
    def _():
        own_gradient()

    pl.semaphore_wait(barrier, 11)

    def tell_xy(r):
        first = (dict(dy=1), dict(dy=NY - 1), dict(dx=1), dict(dx=NX - 1))
        second = (dict(dy=1), dict(dy=NY - 1), dict(dy=2), dict(dy=NY - 2))
        for offset in (first, second)[r]:
            pl.semaphore_signal(near.at[r], inc=1, device_id=at(**offset), device_id_type=MESH)

    def tell_z(r):
        for k in (NZL, 1, NZ - 1):
            pl.semaphore_signal(far.at[r], inc=1, device_id=at(dz=k), device_id_type=MESH)


    def remote(source, goal, send, recv, **offset):
        return pltpu.make_async_remote_copy(
            src_ref=source, dst_ref=goal, send_sem=send, recv_sem=recv,
            device_id=at(**offset), device_id_type=MESH,
        )

    def block_copy(k, kind):
        source, goal = (
            (out_a.at[k], pool_a.at[pl.ds(own * 8, 8)]),
            (out_tail.at[k], pool_tail.at[own]),
            (out_b.at[k], pool_b.at[pl.ds(own * 8, 8)]),
            (out_c.at[k], pool_c.at[pl.ds(own * 8, 8)]),
        )[kind]
        return remote(source, goal, a_send.at[kind], a_recv.at[kind], dz=NZL * (k // 2), dc=k % 2)

    def all_blocks(kind):
        whole = (
            pool_a.at[pl.ds(0, 24)], pool_tail.at[pl.ds(0, 3)],
            pool_b.at[pl.ds(0, 24)], pool_c.at[pl.ds(0, 24)],
        )[kind]
        return remote(whole, whole, a_send.at[kind], a_recv.at[kind], dc=1)

    def send_blocks_of(kinds):
        for k in (2, 3):
            for kind in kinds:
                block_copy(k, kind).start()

    send_blocks_of((0, 1))

    @pl.when(zh == 1)
    def _():
        send_blocks_of((2,))

    for kind in range(4):
        block_copy(1, kind).start()

    tell_xy(0)

    @pl.when(zh == 1)
    def _():
        own_gradient()

    def away(k):
        return 4 + lax.div(k, 2) * (1 - 2 * lax.rem(k, 2)) - lax.rem(k, 2)

    def core_copy(dy):
        return remote(
            part.at[1 - c, lax.rem(y + dy, NY)], given.at[dy], d_send.at[0], d_recv.at[dy], dc=1
        )

    def x_copy(dx, dy):
        return remote(
            chip.at[dy, lax.rem(x + dx, NX), pl.ds(0, XROWS)], from_x.at[dy, dx - 1],
            x_send.at[0], x_recv.at[dy], dx=dx,
        )

    def y_copy(dy):
        return remote(sum_x.at[dy], from_y.at[dy], y_send.at[0], y_recv.at[0], dy=dy)

    def u_copy(dy):
        return remote(
            chip.at[dy, :, pl.ds(XROWS, ROWS - XROWS)], last_y.at[dy], u_send.at[0], u_recv.at[0], dy=dy
        )

    def v_copy(dx):
        return remote(sum_y.at[lax.rem(x + dx, NX)], last_x.at[dx - 1], v_send.at[0], v_recv.at[0], dx=dx)

    def all_of(whole, send, recv):
        return remote(whole, whole, send, recv, dc=1)

    all_x = all_of(from_x, x_send.at[0], x_recv.at[0])
    all_y = all_of(from_y.at[pl.ds(1, NY - 1)], y_send.at[0], y_recv.at[0])
    all_u = all_of(last_y.at[pl.ds(1, NY - 1)], u_send.at[0], u_recv.at[0])
    all_v = all_of(last_x, v_send.at[0], v_recv.at[0])

    def start_core(k, carry):
        core_copy(away(k)).start()
        return carry

    lax.fori_loop(0, NY, start_core, 0)
    tell_z(0)

    def send_x(k):
        dy = away(k)
        for dx in (2, 1, 3):
            x_copy(dx, dy).start()

    def over_cores(k, carry):
        dy = away(k)
        core_copy(dy).wait_recv()
        chip[dy] = part[c, lax.rem(y + dy, NY)] + given[dy]

        @pl.when(k == 0)
        def _():
            pl.semaphore_wait(near.at[0], 4)
            tell_xy(1)

        @pl.when(k > 0)
        def _():
            send_x(k - 1)

        @pl.when(k == 2)
        def _():
            pl.semaphore_wait(near.at[1], 4)

        @pl.when((k == 3) | (k == 4))
        def _():
            u_copy(away(2 * k - 6)).start()
            u_copy(away(2 * k - 5)).start()

        @pl.when(k > 4)
        def _():
            u_copy(away(k - 1)).start()

        return carry

    lax.fori_loop(0, NY, over_cores, 0)
    send_x(NY - 1)

    def send_y(k):
        dy = away(k)

        @pl.when(dy > 0)
        def _():
            y_copy(dy).start()

    def over_x(k, carry):
        dy = away(k)
        all_of(from_x.at[dy], x_send.at[0], x_recv.at[dy]).wait_recv()
        sum_x[dy] = chip[dy, x, :XROWS] + from_x[dy, 0] + from_x[dy, 1] + from_x[dy, 2]

        @pl.when(k > 0)
        def _():
            send_y(k - 1)

        @pl.when(k == 3)
        def _():
            pl.semaphore_wait(far.at[0], 3)
            tell_z(1)

        return carry

    lax.fori_loop(0, NY, over_x, 0)

    rest = chip[0, :, XROWS:]
    all_u.wait_recv()
    for dy in range(1, NY):
        rest = rest + last_y[dy]
    sum_y[...] = rest

    result = sum_x[0]
    for dx in (2, 1, 3):
        v_copy(dx).start()
    all_y.wait_recv()
    for dy in range(1, NY):
        result = result + from_y[dy]
    total[:XROWS] = result
    rest = sum_y[x]
    all_v.wait_recv()
    for dx in range(1, NX):
        rest = rest + last_x[dx - 1]
    total[XROWS:] = rest

    for low in range(NZL):
        for group in range(2):
            tile = total[group * 48 + low * 8 : group * 48 + low * 8 + 8]
            for high in range(NZH):
                to_z[high * NZL + low, :, group * LANES : (group + 1) * LANES] = tile[high * 4 : high * 4 + 4]

    def z_copy(target):
        dz = lax.rem(target - z + NZ, NZ)
        return remote(to_z.at[target], from_z.at[dz], z_send.at[0], z_recv.at[0], dz=dz)

    all_z = all_of(from_z.at[pl.ds(1, NZ - 1)], z_send.at[0], z_recv.at[0])
    from_z[0] = to_z[z]

    pl.semaphore_wait(far.at[1], 3)

    def start_z(target, carry):
        @pl.when(target != z)
        def _():
            z_copy(target).start()

        return carry

    lax.fori_loop(0, NZ, start_z, 0)

    @pl.when(zh == 0)
    def _():
        send_blocks_of((2, 3))

    @pl.when(zh == 1)
    def _():
        send_blocks_of((3,))

    loads[3].wait()
    loads[6].wait()
    for kind in (0, 1):
        all_blocks(kind).wait_recv()
    for shard in range(NZH * NC):
        rows = pool_tail[shard].astype(jnp.float32)
        for j in range(8):
            tails[shard * 8 + j] = jnp.concatenate([rows[4 * j : 4 * j + 4]] * 4, axis=0)

    def first_channels(t, carry):
        def rows(b):
            last = tails[slot_ref[t, b]].astype(jnp.bfloat16)
            return jnp.concatenate([pool_a[slot_ref[t, b]], last], axis=0)

        left = jnp.concatenate([rows(b) for b in range(8)], axis=1)
        right = weights[t].reshape(-1, weights.shape[-1])
        value = jnp.dot(left, right, preferred_element_type=jnp.float32)
        nodes[pl.ds(t, FIRST, stride=8)] = value[:FIRST]
        nodes[pl.ds(MAIN * 8 + t, 4, stride=8)] = value[FIRST : FIRST + 4]
        return carry

    lax.fori_loop(0, 8, first_channels, 0, unroll=True)
    hidden_ref[: FIRST * 8] = nodes[: FIRST * 8].astype(jnp.bfloat16)
    hidden_ref[MAIN * 8 :] = nodes[MAIN * 8 :].astype(jnp.bfloat16)

    def other_channels(p):
        all_blocks(2 + p).wait_recv()
        start, size, pool = ((FIRST, SECOND, pool_b), (FIRST + SECOND, THIRD, pool_c))[p]
        for t in range(8):
            left = jnp.concatenate([pool[slot_ref[t, b]] for b in range(8)], axis=1)
            right = weights[t].reshape(-1, weights.shape[-1])
            nodes[pl.ds(start * 8 + t, size, stride=8)] = jnp.dot(left, right, preferred_element_type=jnp.float32)
        rows = slice(start * 8, (start + size) * 8)
        hidden_ref[rows] = nodes[rows].astype(jnp.bfloat16)

    other_channels(0)

    all_z.wait_recv()
    value = from_z[0]
    for dz in range(1, NZ):
        value = value + from_z[dz]
    for core in range(NC):
        to_core[core] = value[2 * core : 2 * core + 2]

    last_copy = remote(to_core.at[1 - c], from_core, d_send.at[1], d_recv.at[NY], dc=1)
    last_copy.start()
    other_channels(1)

    last_copy.wait_recv()
    mine, other = to_core[c], from_core[...]
    grad_ref[:, :half] = jnp.where(c == 0, mine, other)
    grad_ref[:, half:] = jnp.where(c == 0, other, mine)

    for kind in range(4):
        all_blocks(kind).wait_send()
    all_of(given, d_send.at[0], d_recv.at[0]).wait_send()
    for copies in (all_x, all_y, all_u, all_v, all_z, last_copy):
        copies.wait_send()


def body(field, send_blocks, send_count, regrid_weights, tile_slot, edge_inputs, cotangent):
    tiles, reads, cells, nodes = regrid_weights.shape
    blocks, channels = field.shape[1:3]
    half = cotangent.shape[1] // 2
    field = jnp.transpose(field, (0, 2, 1, 3)).reshape(channels * blocks, cells)
    f32, bf16 = jnp.float32, jnp.bfloat16
    dma = pltpu.SemaphoreType.DMA
    vmem = pl.BlockSpec(memory_space=pltpu.VMEM)
    hbm = pl.BlockSpec(memory_space=pl.ANY)
    hidden, grad = pl.pallas_call(
        kernel,
        name="regrid",
        out_shape=(
            pltpu.VMEM((channels * tiles, nodes), bf16),
            pltpu.VMEM((2, 2 * half), f32),
        ),
        in_specs=[hbm] * 7,
        out_specs=(vmem, vmem),
        scratch_shapes=[
            pltpu.SMEM(send_blocks.shape, jnp.int32),
            pltpu.SMEM(send_count.shape, jnp.int32),
            pltpu.SMEM(tile_slot.shape, jnp.int32),
            pltpu.VMEM(field.shape, bf16),
            pltpu.VMEM((channels * PITCH, cells), f32),
            pltpu.VMEM(regrid_weights.shape, bf16),
            pltpu.VMEM(edge_inputs.shape, bf16),
            pltpu.VMEM(cotangent.shape, bf16),
            pltpu.VMEM((4, 8, FIRST, cells), bf16),
            pltpu.VMEM((4, 8, SECOND, cells), bf16),
            pltpu.VMEM((4, 8, THIRD, cells), bf16),
            pltpu.VMEM((4, 32, cells), bf16),
            pltpu.VMEM((32, FIRST, cells), bf16),
            pltpu.VMEM((32, SECOND, cells), bf16),
            pltpu.VMEM((32, THIRD, cells), bf16),
            pltpu.VMEM((4, 32, cells), bf16),
            pltpu.VMEM((32, 16, cells), f32),
            pltpu.VMEM((channels * tiles, nodes), f32),
            pltpu.VMEM((2, NY, NX, ROWS, LANES), f32),
            pltpu.VMEM((NY, NX, ROWS, LANES), f32),
            pltpu.VMEM((NY, NX, ROWS, LANES), f32),
            pltpu.VMEM((NY, NX - 1, XROWS, LANES), f32),
            pltpu.VMEM((NY, XROWS, LANES), f32),
            pltpu.VMEM((NY, XROWS, LANES), f32),
            pltpu.VMEM((NY, NX, ROWS - XROWS, LANES), f32),
            pltpu.VMEM((NX, ROWS - XROWS, LANES), f32),
            pltpu.VMEM((NX - 1, ROWS - XROWS, LANES), f32),
            pltpu.VMEM((ROWS, LANES), f32),
            pltpu.VMEM((NZ, 4, half), f32),
            pltpu.VMEM((NZ, 4, half), f32),
            pltpu.VMEM((NC, 2, half), f32),
            pltpu.VMEM((2, half), f32),
            pltpu.SemaphoreType.REGULAR((2,)),
            pltpu.SemaphoreType.REGULAR((2,)),
            dma((7,)),
            dma((4,)), dma((4,)),
            dma((2,)), dma((NY + 1,)),
            dma((1,)), dma((NY,)),
            dma((1,)), dma((1,)),
            dma((1,)), dma((1,)),
            dma((1,)), dma((1,)),
            dma((1,)), dma((1,)),
        ],
        compiler_params=pltpu.CompilerParams(
            collective_id=0, has_side_effects=True, vmem_limit_bytes=56 * 2**20
        ),
    )(send_blocks, send_count, tile_slot, field, regrid_weights, edge_inputs, cotangent)
    return jnp.transpose(hidden.reshape(1, channels, tiles, nodes), (0, 2, 1, 3)), grad


def solution(mesh):
    split = Mesh(mesh.devices.reshape(NY, NX, NZL, NZH, NC), AXES)
    rep, sp = AXES[:3], AXES[3:]
    return jax.shard_map(
        body,
        mesh=split,
        in_specs=(
            P(rep, sp, None, None),
            P(sp, None, None),
            P(sp, None),
            P(sp, None, None, None),
            P(sp, None),
            P(AXES, None),
            P(AXES, None),
        ),
        out_specs=(P(rep, sp, None, None), P(AXES, None)),
        check_vma=False,
    )
```

```python
import jax
import jax.numpy as jnp
from jax import lax
from jax.experimental import pallas as pl
from jax.experimental.pallas import tpu as pltpu
from jax.sharding import Mesh
from jax.sharding import PartitionSpec as P

AXES = ("y", "x", "zl", "zh", "c")
NY, NX, NZL, NZH, NC = 8, 4, 6, 2, 2
NZ = NZL * NZH
LANES = 128
ROWS = 96
FIRST, SECOND, THIRD = 64, 16, 16
MAIN = FIRST + SECOND + THIRD
PITCH = 40
XROWS = 80
MESH = pl.DeviceIdType.MESH


def kernel(
    blocks_hbm, count_hbm, slot_hbm, field_hbm, weights_hbm, edges_hbm, cot_hbm,
    hidden_ref, grad_ref,
    blocks_ref, count_ref, slot_ref, field, wide, weights, edges, cot,
    out_a, out_b, out_c, out_tail, pool_a, pool_b, pool_c, pool_tail, tails, nodes,
    part, given, chip, from_x, sum_x, from_y, last_y, sum_y, last_x, total, to_z, from_z, to_core, from_core,
    near, far, in_sem, a_send, a_recv, d_send, d_recv, x_send, x_recv, y_send, y_recv,
    u_send, u_recv, v_send, v_recv, z_send, z_recv,
):
    y, x = lax.axis_index("y"), lax.axis_index("x")
    zl, zh, c = lax.axis_index("zl"), lax.axis_index("zh"), lax.axis_index("c")
    z = zh * NZL + zl
    own = zh * NC + c
    half = cot.shape[1] // 2

    def at(dy=0, dx=0, dz=0, dc=0):
        other = lax.rem(z + dz, NZ)
        return (
            lax.rem(y + dy, NY), lax.rem(x + dx, NX),
            lax.rem(other, NZL), lax.div(other, NZL), lax.rem(c + dc, NC),
        )

    loads = [
        pltpu.make_async_copy(source, goal, in_sem.at[k])
        for k, (source, goal) in enumerate(
            (
                (field_hbm, field), (edges_hbm, edges), (cot_hbm, cot), (weights_hbm, weights),
                (blocks_hbm, blocks_ref), (count_hbm, count_ref), (slot_hbm, slot_ref),
            )
        )
    ]

    barrier = pltpu.get_barrier_semaphore()

    def greet(**offset):
        pl.semaphore_signal(barrier, inc=1, device_id=at(**offset), device_id_type=MESH)

    greet(dz=NZL)
    greet(dz=NZL, dc=1)
    for load in loads:
        load.start()
    for k in (1, NZ - 1):
        greet(dz=k)
        greet(dz=k, dc=1)
    for k in (1, NY - 1):
        greet(dy=k)
    for k in (1, NX - 1):
        greet(dx=k)
    greet(dc=1)

    for k in (0, 4, 5):
        loads[k].wait()

    def widen(k, carry):
        for i in range(10):
            row = k * 10 + i
            wide[pl.ds(pl.multiple_of(row * PITCH, 8), 32)] = field[pl.ds(pl.multiple_of(row * 32, 32), 32)].astype(
                jnp.float32
            )
        return carry

    lax.fori_loop(0, 10, widen, 0)

    def gather(i, carry):
        k = lax.rem(i + 2, 4)
        shard = lax.rem(zh + lax.div(k, 2), NZH) * NC + lax.rem(c + lax.rem(k, 2), NC)
        last = []
        for j in range(8):
            start = blocks_ref[0, shard, j]
            alive = j < count_ref[0, shard]
            main = wide[pl.ds(start, MAIN, stride=PITCH)]
            main = jnp.where(alive, main, jnp.zeros_like(main)).astype(jnp.bfloat16)
            out_a[k, j] = main[:FIRST]
            out_b[k, j] = main[FIRST : FIRST + SECOND]
            out_c[k, j] = main[FIRST + SECOND :]
            tail = wide[pl.ds(start + MAIN * PITCH, 4, stride=PITCH)]
            last.append(jnp.where(alive, tail, jnp.zeros_like(tail)))
        out_tail[k] = jnp.concatenate(last, axis=0).astype(jnp.bfloat16)
        return carry

    lax.fori_loop(0, 4, gather, 0)
    pool_a[pl.ds(own * 8, 8)] = out_a[0]
    pool_b[pl.ds(own * 8, 8)] = out_b[0]
    pool_c[pl.ds(own * 8, 8)] = out_c[0]
    pool_tail[own] = out_tail[0]

    def own_gradient():
        loads[1].wait()
        loads[2].wait()
        for k in range(4):
            piece = lax.dot_general(
                edges[:, k * 384 : (k + 1) * 384], cot[...], (((0,), (0,)), ((), ())),
                preferred_element_type=jnp.float32,
            )
            for h in range(2):
                for g in range(2):
                    column = h * half + g * LANES
                    part[h, 2 * k : 2 * k + 2, :, g * 48 : g * 48 + 48] = piece[:, column : column + LANES].reshape(
                        2, NX, 48, LANES
                    )

    @pl.when(zh == 0)
    def _():
        own_gradient()

    pl.semaphore_wait(barrier, 11)

    def tell_xy(r):
        first = (dict(dy=1), dict(dy=NY - 1), dict(dx=1), dict(dx=NX - 1))
        second = (dict(dy=1), dict(dy=NY - 1), dict(dy=2), dict(dy=NY - 2))
        for offset in (first, second)[r]:
            pl.semaphore_signal(near.at[r], inc=1, device_id=at(**offset), device_id_type=MESH)

    def tell_z(r):
        for k in (NZL, 1, NZ - 1):
            pl.semaphore_signal(far.at[r], inc=1, device_id=at(dz=k), device_id_type=MESH)


    def remote(source, goal, send, recv, **offset):
        return pltpu.make_async_remote_copy(
            src_ref=source, dst_ref=goal, send_sem=send, recv_sem=recv,
            device_id=at(**offset), device_id_type=MESH,
        )

    def block_copy(k, kind):
        source, goal = (
            (out_a.at[k], pool_a.at[pl.ds(own * 8, 8)]),
            (out_tail.at[k], pool_tail.at[own]),
            (out_b.at[k], pool_b.at[pl.ds(own * 8, 8)]),
            (out_c.at[k], pool_c.at[pl.ds(own * 8, 8)]),
        )[kind]
        return remote(source, goal, a_send.at[kind], a_recv.at[kind], dz=NZL * (k // 2), dc=k % 2)

    def all_blocks(kind):
        whole = (
            pool_a.at[pl.ds(0, 24)], pool_tail.at[pl.ds(0, 3)],
            pool_b.at[pl.ds(0, 24)], pool_c.at[pl.ds(0, 24)],
        )[kind]
        return remote(whole, whole, a_send.at[kind], a_recv.at[kind], dc=1)

    def send_blocks_of(kinds):
        for k in (2, 3):
            for kind in kinds:
                block_copy(k, kind).start()

    send_blocks_of((0, 1))

    @pl.when(zh == 1)
    def _():
        send_blocks_of((2,))

    for kind in range(4):
        block_copy(1, kind).start()

    tell_xy(0)

    @pl.when(zh == 1)
    def _():
        own_gradient()

    def away(k):
        return 4 + lax.div(k, 2) * (1 - 2 * lax.rem(k, 2)) - lax.rem(k, 2)

    def core_copy(dy):
        return remote(
            part.at[1 - c, lax.rem(y + dy, NY)], given.at[dy], d_send.at[0], d_recv.at[dy], dc=1
        )

    def x_copy(dx, dy):
        return remote(
            chip.at[dy, lax.rem(x + dx, NX), pl.ds(0, XROWS)], from_x.at[dy, dx - 1],
            x_send.at[0], x_recv.at[dy], dx=dx,
        )

    def y_copy(dy):
        return remote(sum_x.at[dy], from_y.at[dy], y_send.at[0], y_recv.at[0], dy=dy)

    def u_copy(dy):
        return remote(
            chip.at[dy, :, pl.ds(XROWS, ROWS - XROWS)], last_y.at[dy], u_send.at[0], u_recv.at[0], dy=dy
        )

    def v_copy(dx):
        return remote(sum_y.at[lax.rem(x + dx, NX)], last_x.at[dx - 1], v_send.at[0], v_recv.at[0], dx=dx)

    def all_of(whole, send, recv):
        return remote(whole, whole, send, recv, dc=1)

    all_x = all_of(from_x, x_send.at[0], x_recv.at[0])
    all_y = all_of(from_y.at[pl.ds(1, NY - 1)], y_send.at[0], y_recv.at[0])
    all_u = all_of(last_y.at[pl.ds(1, NY - 1)], u_send.at[0], u_recv.at[0])
    all_v = all_of(last_x, v_send.at[0], v_recv.at[0])

    def start_core(k, carry):
        core_copy(away(k)).start()
        return carry

    lax.fori_loop(0, NY, start_core, 0)
    tell_z(0)

    def send_x(k):
        dy = away(k)
        for dx in (2, 1, 3):
            x_copy(dx, dy).start()

    def over_cores(k, carry):
        dy = away(k)
        core_copy(dy).wait_recv()
        chip[dy] = part[c, lax.rem(y + dy, NY)] + given[dy]

        @pl.when(k == 0)
        def _():
            pl.semaphore_wait(near.at[0], 4)
            tell_xy(1)

        @pl.when(k > 0)
        def _():
            send_x(k - 1)

        @pl.when(k == 2)
        def _():
            pl.semaphore_wait(near.at[1], 4)

        @pl.when((k == 3) | (k == 4))
        def _():
            u_copy(away(2 * k - 6)).start()
            u_copy(away(2 * k - 5)).start()

        @pl.when(k > 4)
        def _():
            u_copy(away(k - 1)).start()

        return carry

    lax.fori_loop(0, NY, over_cores, 0)
    send_x(NY - 1)

    def send_y(k):
        dy = away(k)

        @pl.when(dy > 0)
        def _():
            y_copy(dy).start()

    def over_x(k, carry):
        dy = away(k)
        all_of(from_x.at[dy], x_send.at[0], x_recv.at[dy]).wait_recv()
        sum_x[dy] = chip[dy, x, :XROWS] + from_x[dy, 0] + from_x[dy, 1] + from_x[dy, 2]

        @pl.when(k > 0)
        def _():
            send_y(k - 1)

        @pl.when(k == 3)
        def _():
            pl.semaphore_wait(far.at[0], 3)
            tell_z(1)

        return carry

    lax.fori_loop(0, NY, over_x, 0)

    rest = chip[0, :, XROWS:]
    all_u.wait_recv()
    for dy in range(1, NY):
        rest = rest + last_y[dy]
    sum_y[...] = rest

    result = sum_x[0]
    for dx in (2, 1, 3):
        v_copy(dx).start()
    all_y.wait_recv()
    for dy in range(1, NY):
        result = result + from_y[dy]
    total[:XROWS] = result
    rest = sum_y[x]
    all_v.wait_recv()
    for dx in range(1, NX):
        rest = rest + last_x[dx - 1]
    total[XROWS:] = rest

    for low in range(NZL):
        for group in range(2):
            tile = total[group * 48 + low * 8 : group * 48 + low * 8 + 8]
            for high in range(NZH):
                to_z[high * NZL + low, :, group * LANES : (group + 1) * LANES] = tile[high * 4 : high * 4 + 4]

    def z_copy(target):
        dz = lax.rem(target - z + NZ, NZ)
        return remote(to_z.at[target], from_z.at[dz], z_send.at[0], z_recv.at[0], dz=dz)

    all_z = all_of(from_z.at[pl.ds(1, NZ - 1)], z_send.at[0], z_recv.at[0])
    from_z[0] = to_z[z]

    pl.semaphore_wait(far.at[1], 3)

    def start_z(target, carry):
        @pl.when(target != z)
        def _():
            z_copy(target).start()

        return carry

    lax.fori_loop(0, NZL, start_z, 0)

    @pl.when(zh == 1)
    def _():
        send_blocks_of((3,))

    lax.fori_loop(NZL, NZ, start_z, 0)

    @pl.when(zh == 0)
    def _():
        send_blocks_of((2, 3))

    loads[3].wait()
    loads[6].wait()
    for kind in (0, 1):
        all_blocks(kind).wait_recv()
    for shard in range(NZH * NC):
        rows = pool_tail[shard].astype(jnp.float32)
        for j in range(8):
            tails[shard * 8 + j] = jnp.concatenate([rows[4 * j : 4 * j + 4]] * 4, axis=0)

    def first_channels(t, carry):
        def rows(b):
            last = tails[slot_ref[t, b]].astype(jnp.bfloat16)
            return jnp.concatenate([pool_a[slot_ref[t, b]], last], axis=0)

        left = jnp.concatenate([rows(b) for b in range(8)], axis=1)
        right = weights[t].reshape(-1, weights.shape[-1])
        value = jnp.dot(left, right, preferred_element_type=jnp.float32)
        nodes[pl.ds(t, FIRST, stride=8)] = value[:FIRST]
        nodes[pl.ds(MAIN * 8 + t, 4, stride=8)] = value[FIRST : FIRST + 4]
        return carry

    lax.fori_loop(0, 8, first_channels, 0, unroll=True)
    hidden_ref[: FIRST * 8] = nodes[: FIRST * 8].astype(jnp.bfloat16)
    hidden_ref[MAIN * 8 :] = nodes[MAIN * 8 :].astype(jnp.bfloat16)

    def other_channels(p):
        all_blocks(2 + p).wait_recv()
        start, size, pool = ((FIRST, SECOND, pool_b), (FIRST + SECOND, THIRD, pool_c))[p]
        for t in range(8):
            left = jnp.concatenate([pool[slot_ref[t, b]] for b in range(8)], axis=1)
            right = weights[t].reshape(-1, weights.shape[-1])
            nodes[pl.ds(start * 8 + t, size, stride=8)] = jnp.dot(left, right, preferred_element_type=jnp.float32)
        rows = slice(start * 8, (start + size) * 8)
        hidden_ref[rows] = nodes[rows].astype(jnp.bfloat16)

    other_channels(0)

    all_z.wait_recv()
    value = from_z[0]
    for dz in range(1, NZ):
        value = value + from_z[dz]
    for core in range(NC):
        to_core[core] = value[2 * core : 2 * core + 2]

    last_copy = remote(to_core.at[1 - c], from_core, d_send.at[1], d_recv.at[NY], dc=1)
    last_copy.start()
    other_channels(1)

    last_copy.wait_recv()
    mine, other = to_core[c], from_core[...]
    grad_ref[:, :half] = jnp.where(c == 0, mine, other)
    grad_ref[:, half:] = jnp.where(c == 0, other, mine)

    for kind in range(4):
        all_blocks(kind).wait_send()
    all_of(given, d_send.at[0], d_recv.at[0]).wait_send()
    for copies in (all_x, all_y, all_u, all_v, all_z, last_copy):
        copies.wait_send()


def body(field, send_blocks, send_count, regrid_weights, tile_slot, edge_inputs, cotangent):
    tiles, reads, cells, nodes = regrid_weights.shape
    blocks, channels = field.shape[1:3]
    half = cotangent.shape[1] // 2
    field = jnp.transpose(field, (0, 2, 1, 3)).reshape(channels * blocks, cells)
    f32, bf16 = jnp.float32, jnp.bfloat16
    dma = pltpu.SemaphoreType.DMA
    vmem = pl.BlockSpec(memory_space=pltpu.VMEM)
    hbm = pl.BlockSpec(memory_space=pl.ANY)
    hidden, grad = pl.pallas_call(
        kernel,
        name="regrid",
        out_shape=(
            pltpu.VMEM((channels * tiles, nodes), bf16),
            pltpu.VMEM((2, 2 * half), f32),
        ),
        in_specs=[hbm] * 7,
        out_specs=(vmem, vmem),
        scratch_shapes=[
            pltpu.SMEM(send_blocks.shape, jnp.int32),
            pltpu.SMEM(send_count.shape, jnp.int32),
            pltpu.SMEM(tile_slot.shape, jnp.int32),
            pltpu.VMEM(field.shape, bf16),
            pltpu.VMEM((channels * PITCH, cells), f32),
            pltpu.VMEM(regrid_weights.shape, bf16),
            pltpu.VMEM(edge_inputs.shape, bf16),
            pltpu.VMEM(cotangent.shape, bf16),
            pltpu.VMEM((4, 8, FIRST, cells), bf16),
            pltpu.VMEM((4, 8, SECOND, cells), bf16),
            pltpu.VMEM((4, 8, THIRD, cells), bf16),
            pltpu.VMEM((4, 32, cells), bf16),
            pltpu.VMEM((32, FIRST, cells), bf16),
            pltpu.VMEM((32, SECOND, cells), bf16),
            pltpu.VMEM((32, THIRD, cells), bf16),
            pltpu.VMEM((4, 32, cells), bf16),
            pltpu.VMEM((32, 16, cells), f32),
            pltpu.VMEM((channels * tiles, nodes), f32),
            pltpu.VMEM((2, NY, NX, ROWS, LANES), f32),
            pltpu.VMEM((NY, NX, ROWS, LANES), f32),
            pltpu.VMEM((NY, NX, ROWS, LANES), f32),
            pltpu.VMEM((NY, NX - 1, XROWS, LANES), f32),
            pltpu.VMEM((NY, XROWS, LANES), f32),
            pltpu.VMEM((NY, XROWS, LANES), f32),
            pltpu.VMEM((NY, NX, ROWS - XROWS, LANES), f32),
            pltpu.VMEM((NX, ROWS - XROWS, LANES), f32),
            pltpu.VMEM((NX - 1, ROWS - XROWS, LANES), f32),
            pltpu.VMEM((ROWS, LANES), f32),
            pltpu.VMEM((NZ, 4, half), f32),
            pltpu.VMEM((NZ, 4, half), f32),
            pltpu.VMEM((NC, 2, half), f32),
            pltpu.VMEM((2, half), f32),
            pltpu.SemaphoreType.REGULAR((2,)),
            pltpu.SemaphoreType.REGULAR((2,)),
            dma((7,)),
            dma((4,)), dma((4,)),
            dma((2,)), dma((NY + 1,)),
            dma((1,)), dma((NY,)),
            dma((1,)), dma((1,)),
            dma((1,)), dma((1,)),
            dma((1,)), dma((1,)),
            dma((1,)), dma((1,)),
        ],
        compiler_params=pltpu.CompilerParams(
            collective_id=0, has_side_effects=True, vmem_limit_bytes=56 * 2**20
        ),
    )(send_blocks, send_count, tile_slot, field, regrid_weights, edge_inputs, cotangent)
    return jnp.transpose(hidden.reshape(1, channels, tiles, nodes), (0, 2, 1, 3)), grad


def solution(mesh):
    split = Mesh(mesh.devices.reshape(NY, NX, NZL, NZH, NC), AXES)
    rep, sp = AXES[:3], AXES[3:]
    return jax.shard_map(
        body,
        mesh=split,
        in_specs=(
            P(rep, sp, None, None),
            P(sp, None, None),
            P(sp, None),
            P(sp, None, None, None),
            P(sp, None),
            P(AXES, None),
            P(AXES, None),
        ),
        out_specs=(P(rep, sp, None, None), P(AXES, None)),
        check_vma=False,
    )
```

```python
import jax
import jax.numpy as jnp
from jax import lax
from jax.experimental import pallas as pl
from jax.experimental.pallas import tpu as pltpu
from jax.sharding import Mesh
from jax.sharding import PartitionSpec as P

AXES = ("y", "x", "zl", "zh", "c")
NY, NX, NZL, NZH, NC = 8, 4, 6, 2, 2
NZ = NZL * NZH
LANES = 128
ROWS = 96
FIRST, SECOND, THIRD = 64, 16, 16
MAIN = FIRST + SECOND + THIRD
PITCH = 40
XROWS = 72
MESH = pl.DeviceIdType.MESH


def kernel(
    blocks_hbm, count_hbm, slot_hbm, field_hbm, weights_hbm, edges_hbm, cot_hbm,
    hidden_ref, grad_ref,
    blocks_ref, count_ref, slot_ref, field, wide, weights, edges, cot,
    out_a, out_b, out_c, out_tail, pool_a, pool_b, pool_c, pool_tail, tails, nodes,
    part, given, chip, from_x, sum_x, from_y, last_y, sum_y, last_x, total, to_z, from_z, to_core, from_core,
    near, far, in_sem, a_send, a_recv, d_send, d_recv, x_send, x_recv, y_send, y_recv,
    u_send, u_recv, v_send, v_recv, z_send, z_recv,
):
    y, x = lax.axis_index("y"), lax.axis_index("x")
    zl, zh, c = lax.axis_index("zl"), lax.axis_index("zh"), lax.axis_index("c")
    z = zh * NZL + zl
    own = zh * NC + c
    half = cot.shape[1] // 2

    def at(dy=0, dx=0, dz=0, dc=0):
        other = lax.rem(z + dz, NZ)
        return (
            lax.rem(y + dy, NY), lax.rem(x + dx, NX),
            lax.rem(other, NZL), lax.div(other, NZL), lax.rem(c + dc, NC),
        )

    loads = [
        pltpu.make_async_copy(source, goal, in_sem.at[k])
        for k, (source, goal) in enumerate(
            (
                (field_hbm, field), (edges_hbm, edges), (cot_hbm, cot), (weights_hbm, weights),
                (blocks_hbm, blocks_ref), (count_hbm, count_ref), (slot_hbm, slot_ref),
            )
        )
    ]

    barrier = pltpu.get_barrier_semaphore()

    def greet(**offset):
        pl.semaphore_signal(barrier, inc=1, device_id=at(**offset), device_id_type=MESH)

    greet(dz=NZL)
    greet(dz=NZL, dc=1)
    for load in loads:
        load.start()
    for k in (1, NZ - 1):
        greet(dz=k)
        greet(dz=k, dc=1)
    for k in (1, NY - 1):
        greet(dy=k)
    for k in (1, NX - 1):
        greet(dx=k)
    greet(dc=1)

    for k in (0, 4, 5):
        loads[k].wait()

    def widen(k, carry):
        for i in range(10):
            row = k * 10 + i
            wide[pl.ds(pl.multiple_of(row * PITCH, 8), 32)] = field[pl.ds(pl.multiple_of(row * 32, 32), 32)].astype(
                jnp.float32
            )
        return carry

    lax.fori_loop(0, 10, widen, 0)

    def gather(i, carry):
        k = lax.rem(i + 2, 4)
        shard = lax.rem(zh + lax.div(k, 2), NZH) * NC + lax.rem(c + lax.rem(k, 2), NC)
        last = []
        for j in range(8):
            start = blocks_ref[0, shard, j]
            alive = j < count_ref[0, shard]
            main = wide[pl.ds(start, MAIN, stride=PITCH)]
            main = jnp.where(alive, main, jnp.zeros_like(main)).astype(jnp.bfloat16)
            out_a[k, j] = main[:FIRST]
            out_b[k, j] = main[FIRST : FIRST + SECOND]
            out_c[k, j] = main[FIRST + SECOND :]
            tail = wide[pl.ds(start + MAIN * PITCH, 4, stride=PITCH)]
            last.append(jnp.where(alive, tail, jnp.zeros_like(tail)))
        out_tail[k] = jnp.concatenate(last, axis=0).astype(jnp.bfloat16)
        return carry

    lax.fori_loop(0, 4, gather, 0)
    pool_a[pl.ds(own * 8, 8)] = out_a[0]
    pool_b[pl.ds(own * 8, 8)] = out_b[0]
    pool_c[pl.ds(own * 8, 8)] = out_c[0]
    pool_tail[own] = out_tail[0]

    def own_gradient():
        loads[1].wait()
        loads[2].wait()
        for k in range(4):
            piece = lax.dot_general(
                edges[:, k * 384 : (k + 1) * 384], cot[...], (((0,), (0,)), ((), ())),
                preferred_element_type=jnp.float32,
            )
            for h in range(2):
                for g in range(2):
                    column = h * half + g * LANES
                    part[h, 2 * k : 2 * k + 2, :, g * 48 : g * 48 + 48] = piece[:, column : column + LANES].reshape(
                        2, NX, 48, LANES
                    )

    @pl.when(zh == 0)
    def _():
        own_gradient()

    pl.semaphore_wait(barrier, 11)

    def tell_xy(r):
        first = (dict(dy=1), dict(dy=NY - 1), dict(dx=1), dict(dx=NX - 1))
        second = (dict(dy=1), dict(dy=NY - 1), dict(dy=2), dict(dy=NY - 2))
        for offset in (first, second)[r]:
            pl.semaphore_signal(near.at[r], inc=1, device_id=at(**offset), device_id_type=MESH)

    def tell_z(r):
        for k in (NZL, 1, NZ - 1):
            pl.semaphore_signal(far.at[r], inc=1, device_id=at(dz=k), device_id_type=MESH)


    def remote(source, goal, send, recv, **offset):
        return pltpu.make_async_remote_copy(
            src_ref=source, dst_ref=goal, send_sem=send, recv_sem=recv,
            device_id=at(**offset), device_id_type=MESH,
        )

    def block_copy(k, kind):
        source, goal = (
            (out_a.at[k], pool_a.at[pl.ds(own * 8, 8)]),
            (out_tail.at[k], pool_tail.at[own]),
            (out_b.at[k], pool_b.at[pl.ds(own * 8, 8)]),
            (out_c.at[k], pool_c.at[pl.ds(own * 8, 8)]),
        )[kind]
        return remote(source, goal, a_send.at[kind], a_recv.at[kind], dz=NZL * (k // 2), dc=k % 2)

    def all_blocks(kind):
        whole = (
            pool_a.at[pl.ds(0, 24)], pool_tail.at[pl.ds(0, 3)],
            pool_b.at[pl.ds(0, 24)], pool_c.at[pl.ds(0, 24)],
        )[kind]
        return remote(whole, whole, a_send.at[kind], a_recv.at[kind], dc=1)

    def send_blocks_of(kinds):
        for k in (2, 3):
            for kind in kinds:
                block_copy(k, kind).start()

    send_blocks_of((0, 1))

    @pl.when(zh == 1)
    def _():
        send_blocks_of((2,))

    for kind in range(4):
        block_copy(1, kind).start()

    tell_xy(0)

    @pl.when(zh == 1)
    def _():
        own_gradient()

    def away(k):
        return 4 + lax.div(k, 2) * (1 - 2 * lax.rem(k, 2)) - lax.rem(k, 2)

    def core_copy(dy):
        return remote(
            part.at[1 - c, lax.rem(y + dy, NY)], given.at[dy], d_send.at[0], d_recv.at[dy], dc=1
        )

    def x_copy(dx, dy):
        return remote(
            chip.at[dy, lax.rem(x + dx, NX), pl.ds(0, XROWS)], from_x.at[dy, dx - 1],
            x_send.at[0], x_recv.at[dy], dx=dx,
        )

    def y_copy(dy):
        return remote(sum_x.at[dy], from_y.at[dy], y_send.at[0], y_recv.at[0], dy=dy)

    def u_copy(dy):
        return remote(
            chip.at[dy, :, pl.ds(XROWS, ROWS - XROWS)], last_y.at[dy], u_send.at[0], u_recv.at[0], dy=dy
        )

    def v_copy(dx):
        return remote(sum_y.at[lax.rem(x + dx, NX)], last_x.at[dx - 1], v_send.at[0], v_recv.at[0], dx=dx)

    def all_of(whole, send, recv):
        return remote(whole, whole, send, recv, dc=1)

    all_x = all_of(from_x, x_send.at[0], x_recv.at[0])
    all_y = all_of(from_y.at[pl.ds(1, NY - 1)], y_send.at[0], y_recv.at[0])
    all_u = all_of(last_y.at[pl.ds(1, NY - 1)], u_send.at[0], u_recv.at[0])
    all_v = all_of(last_x, v_send.at[0], v_recv.at[0])

    def start_core(k, carry):
        core_copy(away(k)).start()
        return carry

    lax.fori_loop(0, NY, start_core, 0)
    tell_z(0)

    def send_x(k):
        dy = away(k)
        for dx in (2, 1, 3):
            x_copy(dx, dy).start()

    def over_cores(k, carry):
        dy = away(k)
        core_copy(dy).wait_recv()
        chip[dy] = part[c, lax.rem(y + dy, NY)] + given[dy]

        @pl.when(k == 0)
        def _():
            pl.semaphore_wait(near.at[0], 4)
            tell_xy(1)

        @pl.when(k > 0)
        def _():
            send_x(k - 1)

        @pl.when(k == 2)
        def _():
            pl.semaphore_wait(near.at[1], 4)

        @pl.when((k == 3) | (k == 4))
        def _():
            u_copy(away(2 * k - 6)).start()
            u_copy(away(2 * k - 5)).start()

        @pl.when(k > 4)
        def _():
            u_copy(away(k - 1)).start()

        return carry

    lax.fori_loop(0, NY, over_cores, 0)
    send_x(NY - 1)

    def send_y(k):
        dy = away(k)

        @pl.when(dy > 0)
        def _():
            y_copy(dy).start()

    def over_x(k, carry):
        dy = away(k)
        all_of(from_x.at[dy], x_send.at[0], x_recv.at[dy]).wait_recv()
        sum_x[dy] = chip[dy, x, :XROWS] + from_x[dy, 0] + from_x[dy, 1] + from_x[dy, 2]

        @pl.when(k > 0)
        def _():
            send_y(k - 1)

        @pl.when(k == 3)
        def _():
            pl.semaphore_wait(far.at[0], 3)
            tell_z(1)

        return carry

    lax.fori_loop(0, NY, over_x, 0)

    rest = chip[0, :, XROWS:]
    all_u.wait_recv()
    for dy in range(1, NY):
        rest = rest + last_y[dy]
    sum_y[...] = rest

    result = sum_x[0]
    for dx in (2, 1, 3):
        v_copy(dx).start()
    all_y.wait_recv()
    for dy in range(1, NY):
        result = result + from_y[dy]
    total[:XROWS] = result
    rest = sum_y[x]
    all_v.wait_recv()
    for dx in range(1, NX):
        rest = rest + last_x[dx - 1]
    total[XROWS:] = rest

    for low in range(NZL):
        for group in range(2):
            tile = total[group * 48 + low * 8 : group * 48 + low * 8 + 8]
            for high in range(NZH):
                to_z[high * NZL + low, :, group * LANES : (group + 1) * LANES] = tile[high * 4 : high * 4 + 4]

    def z_copy(target):
        dz = lax.rem(target - z + NZ, NZ)
        return remote(to_z.at[target], from_z.at[dz], z_send.at[0], z_recv.at[0], dz=dz)

    all_z = all_of(from_z.at[pl.ds(1, NZ - 1)], z_send.at[0], z_recv.at[0])
    from_z[0] = to_z[z]

    pl.semaphore_wait(far.at[1], 3)

    def start_z(target, carry):
        @pl.when(target != z)
        def _():
            z_copy(target).start()

        return carry

    lax.fori_loop(0, NZ, start_z, 0)

    @pl.when(zh == 0)
    def _():
        send_blocks_of((2, 3))

    @pl.when(zh == 1)
    def _():
        send_blocks_of((3,))

    loads[3].wait()
    loads[6].wait()
    for kind in (0, 1):
        all_blocks(kind).wait_recv()
    for shard in range(NZH * NC):
        rows = pool_tail[shard].astype(jnp.float32)
        for j in range(8):
            tails[shard * 8 + j] = jnp.concatenate([rows[4 * j : 4 * j + 4]] * 4, axis=0)

    def first_channels(t, carry):
        def rows(b):
            last = tails[slot_ref[t, b]].astype(jnp.bfloat16)
            return jnp.concatenate([pool_a[slot_ref[t, b]], last], axis=0)

        left = jnp.concatenate([rows(b) for b in range(8)], axis=1)
        right = weights[t].reshape(-1, weights.shape[-1])
        value = jnp.dot(left, right, preferred_element_type=jnp.float32)
        nodes[pl.ds(t, FIRST, stride=8)] = value[:FIRST]
        nodes[pl.ds(MAIN * 8 + t, 4, stride=8)] = value[FIRST : FIRST + 4]
        return carry

    lax.fori_loop(0, 8, first_channels, 0, unroll=True)
    hidden_ref[: FIRST * 8] = nodes[: FIRST * 8].astype(jnp.bfloat16)
    hidden_ref[MAIN * 8 :] = nodes[MAIN * 8 :].astype(jnp.bfloat16)

    def other_channels(p):
        all_blocks(2 + p).wait_recv()
        start, size, pool = ((FIRST, SECOND, pool_b), (FIRST + SECOND, THIRD, pool_c))[p]
        for t in range(8):
            left = jnp.concatenate([pool[slot_ref[t, b]] for b in range(8)], axis=1)
            right = weights[t].reshape(-1, weights.shape[-1])
            nodes[pl.ds(start * 8 + t, size, stride=8)] = jnp.dot(left, right, preferred_element_type=jnp.float32)
        rows = slice(start * 8, (start + size) * 8)
        hidden_ref[rows] = nodes[rows].astype(jnp.bfloat16)

    other_channels(0)

    all_z.wait_recv()
    value = from_z[0]
    for dz in range(1, NZ):
        value = value + from_z[dz]
    for core in range(NC):
        to_core[core] = value[2 * core : 2 * core + 2]

    last_copy = remote(to_core.at[1 - c], from_core, d_send.at[1], d_recv.at[NY], dc=1)
    last_copy.start()
    other_channels(1)

    last_copy.wait_recv()
    mine, other = to_core[c], from_core[...]
    grad_ref[:, :half] = jnp.where(c == 0, mine, other)
    grad_ref[:, half:] = jnp.where(c == 0, other, mine)

    for kind in range(4):
        all_blocks(kind).wait_send()
    all_of(given, d_send.at[0], d_recv.at[0]).wait_send()
    for copies in (all_x, all_y, all_u, all_v, all_z, last_copy):
        copies.wait_send()


def hand_over(hidden_ref, grad_ref, hidden_out, grad_out, sems):
    copies = [
        pltpu.make_async_copy(hidden_ref, hidden_out, sems.at[0]),
        pltpu.make_async_copy(grad_ref, grad_out, sems.at[1]),
    ]
    for copy in copies:
        copy.start()
    for copy in copies:
        copy.wait()


def body(field, send_blocks, send_count, regrid_weights, tile_slot, edge_inputs, cotangent):
    tiles, reads, cells, nodes = regrid_weights.shape
    blocks, channels = field.shape[1:3]
    half = cotangent.shape[1] // 2
    field = jnp.transpose(field, (0, 2, 1, 3)).reshape(channels * blocks, cells)
    f32, bf16 = jnp.float32, jnp.bfloat16
    dma = pltpu.SemaphoreType.DMA
    vmem = pl.BlockSpec(memory_space=pltpu.VMEM)
    hbm = pl.BlockSpec(memory_space=pl.ANY)
    hidden, grad = pl.pallas_call(
        kernel,
        name="regrid",
        out_shape=(
            pltpu.VMEM((channels * tiles, nodes), bf16),
            pltpu.VMEM((2, 2 * half), f32),
        ),
        in_specs=[hbm] * 7,
        out_specs=(vmem, vmem),
        scratch_shapes=[
            pltpu.SMEM(send_blocks.shape, jnp.int32),
            pltpu.SMEM(send_count.shape, jnp.int32),
            pltpu.SMEM(tile_slot.shape, jnp.int32),
            pltpu.VMEM(field.shape, bf16),
            pltpu.VMEM((channels * PITCH, cells), f32),
            pltpu.VMEM(regrid_weights.shape, bf16),
            pltpu.VMEM(edge_inputs.shape, bf16),
            pltpu.VMEM(cotangent.shape, bf16),
            pltpu.VMEM((4, 8, FIRST, cells), bf16),
            pltpu.VMEM((4, 8, SECOND, cells), bf16),
            pltpu.VMEM((4, 8, THIRD, cells), bf16),
            pltpu.VMEM((4, 32, cells), bf16),
            pltpu.VMEM((32, FIRST, cells), bf16),
            pltpu.VMEM((32, SECOND, cells), bf16),
            pltpu.VMEM((32, THIRD, cells), bf16),
            pltpu.VMEM((4, 32, cells), bf16),
            pltpu.VMEM((32, 16, cells), f32),
            pltpu.VMEM((channels * tiles, nodes), f32),
            pltpu.VMEM((2, NY, NX, ROWS, LANES), f32),
            pltpu.VMEM((NY, NX, ROWS, LANES), f32),
            pltpu.VMEM((NY, NX, ROWS, LANES), f32),
            pltpu.VMEM((NY, NX - 1, XROWS, LANES), f32),
            pltpu.VMEM((NY, XROWS, LANES), f32),
            pltpu.VMEM((NY, XROWS, LANES), f32),
            pltpu.VMEM((NY, NX, ROWS - XROWS, LANES), f32),
            pltpu.VMEM((NX, ROWS - XROWS, LANES), f32),
            pltpu.VMEM((NX - 1, ROWS - XROWS, LANES), f32),
            pltpu.VMEM((ROWS, LANES), f32),
            pltpu.VMEM((NZ, 4, half), f32),
            pltpu.VMEM((NZ, 4, half), f32),
            pltpu.VMEM((NC, 2, half), f32),
            pltpu.VMEM((2, half), f32),
            pltpu.SemaphoreType.REGULAR((2,)),
            pltpu.SemaphoreType.REGULAR((2,)),
            dma((7,)),
            dma((4,)), dma((4,)),
            dma((2,)), dma((NY + 1,)),
            dma((1,)), dma((NY,)),
            dma((1,)), dma((1,)),
            dma((1,)), dma((1,)),
            dma((1,)), dma((1,)),
            dma((1,)), dma((1,)),
        ],
        compiler_params=pltpu.CompilerParams(
            collective_id=0, has_side_effects=True, vmem_limit_bytes=56 * 2**20
        ),
    )(send_blocks, send_count, tile_slot, field, regrid_weights, edge_inputs, cotangent)
    hidden, grad = pl.pallas_call(
        hand_over,
        name="hand_over",
        out_shape=(
            jax.ShapeDtypeStruct(hidden.shape, bf16),
            jax.ShapeDtypeStruct(grad.shape, f32),
        ),
        in_specs=[pl.BlockSpec(memory_space=pltpu.VMEM)] * 2,
        out_specs=(hbm, hbm),
        scratch_shapes=[dma((2,))],
    )(
        pltpu.with_memory_space_constraint(hidden, pltpu.VMEM),
        pltpu.with_memory_space_constraint(grad, pltpu.VMEM),
    )
    return jnp.transpose(hidden.reshape(1, channels, tiles, nodes), (0, 2, 1, 3)), grad


def solution(mesh):
    split = Mesh(mesh.devices.reshape(NY, NX, NZL, NZH, NC), AXES)
    rep, sp = AXES[:3], AXES[3:]
    return jax.shard_map(
        body,
        mesh=split,
        in_specs=(
            P(rep, sp, None, None),
            P(sp, None, None),
            P(sp, None),
            P(sp, None, None, None),
            P(sp, None),
            P(AXES, None),
            P(AXES, None),
        ),
        out_specs=(P(rep, sp, None, None), P(AXES, None)),
        check_vma=False,
    )
```
